256 devices in a mesh: seq: 32 (over y, z_lo, x), exp: 8 (over z_hi, core).
Axes of the slice: x: 4, y: 4, z: 8 (z_hi: 4, z_lo: 2; z = z_hi * 2 + z_lo), core: 2. Of those that a mesh axis runs over, the one named last changes fastest.
Arguments:
- query_input: bfloat16 [4096, 2048], P('seq', 'exp'), may hold values from -4.5 to 4.5
- key_input: bfloat16 [4096, 2048], P('seq', 'exp'), may hold values from -4.5 to 4.5
- value_input: bfloat16 [4096, 2048], P('seq', 'exp'), may hold values from -6 to 6
- segment_ids: int32 [4096], P('seq'), may hold values from 0 to 15, never falling along the last dimension, each value on 1 to 512 neighbouring positions
- residual_in: bfloat16 [4096, 4096], P('seq', 'exp'), may hold values from -13.5 to 13.5
- out_weight: bfloat16 [2048, 4096], P('exp'), may hold values from -0.1875 to 0.1875
- norm_gain: float32 [4096], P('exp'), may hold values from 0.1 to 1.9
- router: bfloat16 [4096, 32], P(None, 'seq'), may hold values from -0.1875 to 0.1875
- modality: int32 [4096], P('seq'), may hold values from 0 to 1
- expert_in: int32 [4096], P('seq'), may hold values from 0 to 15, as said below
- gate_weight: bfloat16 [32, 4096, 2816], P('seq', None, 'exp'), may hold values from -0.09375 to 0.09375
- up_weight: bfloat16 [32, 4096, 2816], P('seq', None, 'exp'), may hold values from -0.09375 to 0.09375
- down_weight: bfloat16 [32, 2816, 4096], P('seq', 'exp'), may hold values from -0.15625 to 0.15625
Outputs:
- layer_out: bfloat16 [4096, 4096], P('seq', 'exp')
The draws below stay inside these ranges and needn't reach their ends.
Inputs may be any that keep to these rules, and one draw needn't show every extreme that they name: `segment_ids`: document numbers never fall along the sequence, and a document holds at most an eighth of the 4096 tokens. `expert_in`: within each aligned block of 128 tokens no expert (modality and number together) is chosen by more than 7 tokens, and in every block some expert is chosen by exactly 7.
All inputs are finite; a program needn't handle non-finite values.
Results may differ from the reference program's by a relative error of at most 0.0095.
Values may be sent and summed in bfloat16 or wider, within the bound.
A program may use at most 64 MiB of HBM per device.

```python
import math
import jax
import jax.numpy as jnp
import numpy as np
from jax import lax

D = 4096
FF = 2816
HEADS = 16
HEAD_DIM = 128
EXPERTS = 32
DOCS = 16
TOK = 128
MODAL_EXPERTS = 16
SEQ_LEN = 4096
CAPACITY = 7
FF_DEV = 352
N_SEQ = 32
N_EXP = 8


def routing_choice(key):
    base_key = jax.random.fold_in(key, 101)
    pick_key, count_key, jitter_key, order_key = jax.random.split(base_key, 4)
    block_count = SEQ_LEN // TOK
    hot_experts = jax.random.permutation(pick_key, EXPERTS)[:3]
    is_hot = jnp.zeros((EXPERTS,), jnp.int32).at[hot_experts].set(1)
    lowest = (TOK - 3 * CAPACITY + EXPERTS - 4) // (EXPERTS - 3)
    slot_counts = jax.random.randint(count_key, (block_count, EXPERTS), lowest, CAPACITY)
    slot_counts = jnp.where(is_hot[None, :] == 1, CAPACITY, slot_counts)
    rank_grid = jnp.arange(CAPACITY, dtype=jnp.int32)
    usable = rank_grid[None, None, :] < slot_counts[:, :, None]
    priority = jnp.where(usable, 1 + is_hot[None, :, None], 0)
    jitter = jax.random.randint(jitter_key, (block_count, EXPERTS, CAPACITY), 0, 1024)
    flat_index = jnp.arange(EXPERTS * CAPACITY, dtype=jnp.int32).reshape(EXPERTS, CAPACITY)
    scores = priority * (1 << 25) + jitter * (EXPERTS * CAPACITY) + flat_index[None]
    scores = scores.reshape(block_count, EXPERTS * CAPACITY).astype(jnp.int32)
    ignored_values, chosen = lax.top_k(scores, TOK)
    picked = (chosen // CAPACITY).astype(jnp.int32)
    order_keys = jax.random.split(order_key, block_count)
    shuffled = jax.vmap(jax.random.permutation)(order_keys, picked)
    return shuffled.reshape(SEQ_LEN).astype(jnp.int32)


def draw_modality(key, part):
    return (routing_choice(key) // MODAL_EXPERTS).astype(jnp.int32)


def draw_expert_in(key, part):
    return (routing_choice(key) % MODAL_EXPERTS).astype(jnp.int32)


def drawn_pairs(key):
    base_key = jax.random.fold_in(key, 202)
    query_key, key_key = jax.random.split(base_key, 2)
    columns = HEADS * HEAD_DIM
    query_draw = jnp.clip(jax.random.normal(query_key, (SEQ_LEN, columns), jnp.float32), -4.5, 4.5)
    key_draw = jnp.clip(jax.random.normal(key_key, (SEQ_LEN, columns), jnp.float32), -4.5, 4.5)
    return (query_draw, key_draw)


def draw_query_input(key, part):
    return drawn_pairs(key)[0].astype(jnp.bfloat16)


def draw_key_input(key, part):
    return drawn_pairs(key)[1].astype(jnp.bfloat16)


def draw_residual_in(key, part):
    base_key = jax.random.fold_in(key, 303)
    value_key = jax.random.fold_in(base_key, 0)
    column_ramp = jnp.arange(D, dtype=jnp.float32) / D
    entries = jnp.clip(jax.random.normal(value_key, (SEQ_LEN, D), jnp.float32), -3.0, 3.0) * 0.7 * (3.0 ** column_ramp)[None, :]
    return entries.astype(jnp.bfloat16)


def raised(values, key, source, target, parts, factor):
    def block_of(position):
        return (jnp.arange(values.shape[position]) // (values.shape[position] // parts)).reshape((-1,) + (1,) * (values.ndim - 1 - position))

    first = jax.random.permutation(key, parts)[block_of(target)]
    far = (block_of(target) + parts // 2) % parts
    return jnp.where((block_of(source) == first) | (block_of(source) == far), factor * values, values)


def level_of(key, extent, cuts, low, top_value):
    loudness, own = 1.0, jax.random.fold_in(key, 6)
    for dim, shards_of in cuts:
        draws = jnp.exp(jax.random.uniform(jax.random.fold_in(own, dim), (shards_of,), jnp.float32, low / len(cuts), top_value / len(cuts)))
        loudness = loudness * jnp.repeat(draws, extent[dim] // shards_of).reshape([-1 if axis == dim else 1 for axis in range(len(extent))])
    return loudness


def length_profile(number_of, total, most, slope):
    portions = [(1 << 20) // math.isqrt(rank ** slope) + 1 for rank in range(2, number_of + 1)]
    rest, counts = total - most - (number_of - 1), [1] * (number_of - 1)
    while rest > 0:
        movable = [i for i in range(number_of - 1) if counts[i] < most]
        whole, remaining = sum([portions[i] for i in movable]), rest
        for i in movable:
            addition = min(most - counts[i], max(1, remaining * portions[i] // whole), rest)
            counts[i] = counts[i] + addition
            rest = rest - addition
    return np.array([most] + counts)


def uneven_parts(own_key, number_of, total, reach, slope):
    if number_of == 2:
        one = jax.random.randint(own_key, (), max(1, total - reach), min(reach, total - 1) + 1)
        return jnp.stack([one, total - one])
    lengths = jnp.asarray(length_profile(number_of, total, reach, slope), jnp.int32)
    twos = (number_of - 1) // 2
    giver, sink = lengths[1:1 + 2 * twos:2], lengths[2:2 + 2 * twos:2]
    slack = jnp.minimum(giver - 1, reach - sink)
    shifted = jax.random.randint(jax.random.fold_in(own_key, 1), (twos,), 0, 1 << 20) % (slack + 1)
    lengths = lengths.at[1:1 + 2 * twos:2].set(giver - shifted).at[2:2 + 2 * twos:2].set(sink + shifted)
    return lengths[jax.random.permutation(jax.random.fold_in(own_key, 2), number_of)]


def gaussian(key, shape, deviation, most, cuts=(), held_as=jnp.bfloat16):
    level = level_of(key, shape, cuts, -0.22, 0.18) if cuts else 1.0
    values = jax.random.normal(key, shape, jnp.float32) * deviation * level
    return jnp.minimum(jnp.maximum(values, -most), most).astype(held_as)


def heavy_noise(key, dims, scale, most, shards, heavy, held_as=jnp.bfloat16):
    values = scale * jax.random.normal(key, dims, jnp.float32)
    if shards:
        values = values * level_of(key, dims, shards, -0.22, 0.18)
    return jnp.clip(raised(values, jax.random.fold_in(key, 3), *heavy), -most, most).astype(held_as)


def setup_inputs(seed: int = 0) -> dict:
    splits = jax.random.split(jax.random.key(seed), 14)
    return {
        "query_input": draw_query_input(jax.random.fold_in(splits[13], 71), 0),
        "key_input": draw_key_input(jax.random.fold_in(splits[13], 71), 0),
        "value_input": gaussian(splits[2], (SEQ_LEN, HEADS * HEAD_DIM), 1.0, 6.0, ((0, 32), (1, 8))),
        "segment_ids": jnp.searchsorted(jnp.cumsum(uneven_parts(splits[3], DOCS, SEQ_LEN, SEQ_LEN // 8, 1)), jnp.arange(SEQ_LEN), side="right").astype(jnp.int32),
        "residual_in": draw_residual_in(jax.random.fold_in(splits[13], 71), 0),
        "out_weight": heavy_noise(splits[5], (HEADS * HEAD_DIM, D), (HEADS * HEAD_DIM) ** -0.5, 0.1875, ((0, 8),), (0, 1, 8, 2.0)),
        "norm_gain": jnp.clip(1.0 + 0.18 * jax.random.normal(splits[6], (D,), jnp.float32), 0.1, 1.9),
        "router": gaussian(splits[7], (D, EXPERTS), (D // 4) ** -0.5, 0.1875, ((1, 32),)),
        "modality": draw_modality(jax.random.fold_in(splits[13], 71), 0),
        "expert_in": draw_expert_in(jax.random.fold_in(splits[13], 71), 0),
        "gate_weight": gaussian(splits[10], (EXPERTS, D, FF), D ** -0.5, 0.09375, ((0, 32), (2, 8))),
        "up_weight": gaussian(splits[11], (EXPERTS, D, FF), D ** -0.5, 0.09375, ((0, 32), (2, 8))),
        "down_weight": heavy_noise(splits[12], (EXPERTS, FF, D), FF ** -0.5, 0.15625, ((0, 32), (1, 8)), (1, 2, 8, 2.0)),
    }


NEGATIVE = -1e+30
EPSILON = 1e-05

def attend_block(query_input, key_input, value_input, segment_ids, out_weight, start):
    key_width = SEQ_LEN // 8 + TOK
    key_start = jnp.maximum(start - SEQ_LEN // 8, 0).astype(jnp.int32)
    query_rows = lax.dynamic_slice_in_dim(query_input, start, TOK, 0).astype(jnp.float32).reshape(TOK, HEADS, HEAD_DIM)
    key_rows = lax.dynamic_slice_in_dim(key_input, key_start, key_width, 0).astype(jnp.float32).reshape(key_width, HEADS, HEAD_DIM)
    value_rows = lax.dynamic_slice_in_dim(value_input, key_start, key_width, 0).astype(jnp.float32).reshape(key_width, HEADS, HEAD_DIM)
    query_seg = lax.dynamic_slice_in_dim(segment_ids, start, TOK, 0)
    key_seg = lax.dynamic_slice_in_dim(segment_ids, key_start, key_width, 0)
    query_pos = start + jnp.arange(TOK, dtype=jnp.int32)
    key_pos = key_start + jnp.arange(key_width, dtype=jnp.int32)
    allowed = (query_seg[:, None] == key_seg[None, :]) & (key_pos[None, :] <= query_pos[:, None])
    scores = jnp.einsum('qhd,khd->hqk', query_rows, key_rows) * HEAD_DIM ** (-0.5)
    masked = jnp.where(allowed[None], scores, NEGATIVE)
    peak = lax.optimization_barrier(jnp.max(masked, axis=2, keepdims=True))
    weights = jnp.where(allowed[None], jnp.exp(masked - peak), 0.0)
    denominators = lax.optimization_barrier(jnp.sum(weights, axis=2))
    probabilities = lax.optimization_barrier(weights.astype(jnp.bfloat16)).astype(jnp.float32)
    numerators = jnp.einsum('hqk,khd->qhd', probabilities, value_rows)
    attended = (numerators / jnp.transpose(denominators)[:, :, None]).astype(jnp.bfloat16)
    group_width = HEADS * HEAD_DIM // N_EXP
    attended = attended.reshape(TOK, N_EXP, group_width).astype(jnp.float32)
    pieces = jnp.einsum('tng,ngd->tnd', attended, out_weight.astype(jnp.float32).reshape(N_EXP, group_width, D))
    pieces = lax.optimization_barrier(pieces.astype(jnp.bfloat16)).astype(jnp.float32)
    return lax.optimization_barrier(jnp.sum(pieces, axis=1))

def expert_apply(items):
    expert_rows, gate_part, up_part, down_part, router_column = items
    gate_sum = jnp.dot(expert_rows, gate_part, preferred_element_type=jnp.float32)
    up_sum = jnp.dot(expert_rows, up_part, preferred_element_type=jnp.float32)
    logits = jnp.dot(expert_rows, router_column, preferred_element_type=jnp.float32)
    hidden = (jax.nn.silu(gate_sum) * up_sum * jax.nn.sigmoid(logits)[:, None]).astype(jnp.bfloat16)
    row_count = expert_rows.shape[0]
    pieces = jnp.einsum('rng,ngd->rnd', hidden.astype(jnp.float32).reshape(row_count, N_EXP, FF_DEV), down_part.astype(jnp.float32).reshape(N_EXP, FF_DEV, D))
    pieces = lax.optimization_barrier(pieces.astype(jnp.bfloat16)).astype(jnp.float32)
    return lax.optimization_barrier(jnp.sum(pieces, axis=1)).astype(jnp.bfloat16)

def reference(query_input, key_input, value_input, segment_ids, residual_in, out_weight, norm_gain, router, modality, expert_in, gate_weight, up_weight, down_weight):
    starts = jnp.arange(N_SEQ, dtype=jnp.int32) * TOK

    def one_block(start):
        return attend_block(query_input, key_input, value_input, segment_ids, out_weight, start)
    attention = lax.map(one_block, starts).reshape(SEQ_LEN, D)
    residual = residual_in.astype(jnp.float32) + attention
    norm_scale = lax.rsqrt(lax.optimization_barrier(jnp.sum(residual * residual, axis=1, keepdims=True)) / D + EPSILON)
    normed = (residual * norm_scale * norm_gain).astype(jnp.bfloat16)
    picked = (modality * MODAL_EXPERTS + expert_in).astype(jnp.int32)
    block_picks = picked.reshape(N_SEQ, TOK)
    one_hot = (block_picks[:, :, None] == jnp.arange(EXPERTS, dtype=jnp.int32)[None, None, :]).astype(jnp.int32)
    running = (jnp.cumsum(one_hot, axis=1) - 1).astype(jnp.int32)
    rank_in_block = lax.optimization_barrier(jnp.sum(one_hot * running, axis=2)).astype(jnp.int32)
    slot_index = (jnp.arange(N_SEQ, dtype=jnp.int32)[:, None] * CAPACITY + rank_in_block).reshape(SEQ_LEN).astype(jnp.int32)
    expert_rows = jnp.zeros((EXPERTS, N_SEQ * CAPACITY, D), jnp.bfloat16).at[picked, slot_index].set(normed)
    expert_outputs = lax.map(expert_apply, (expert_rows, gate_weight, up_weight, down_weight, jnp.transpose(router)))
    routed = expert_outputs[picked, slot_index]
    return (residual + routed.astype(jnp.float32)).astype(jnp.bfloat16)
```

```python
import jax
import jax.numpy as jnp
from jax import lax
from jax.experimental import pallas as pl
from jax.experimental.pallas import tpu as pltpu
from jax.sharding import PartitionSpec as P

D = 4096
EPSILON = 1e-05
NEGATIVE = -1e30
TOK = 128
HEAD = 128
WIDE = 256
COLS = 512
HALF = 256
NSEQ = 32
ROWS = 224
SLOTS = 256
UNITS = 352
MESH = pl.DeviceIdType.MESH
F32 = jnp.float32
BF16 = jnp.bfloat16


def dot(a, b):
    return jnp.dot(a, b, preferred_element_type=F32)


def dot_nt(a, b):
    return lax.dot_general(a, b, (((1,), (1,)), ((), ())), preferred_element_type=F32)


def iota(shape, dim):
    return lax.broadcasted_iota(jnp.int32, shape, dim)


def as_column(row):
    return jnp.transpose(jnp.broadcast_to(row, (TOK, TOK)))


def kernel(
    q_hbm, k_hbm, v_hbm, ids_ref, res_hbm, w_hbm, gain_ref, router_ref, gate_hbm, up_hbm, down_hbm,
    out_ref,
    qs, kb, vb, sb, res, w2, gu, d2, att, r1s, r1r, ss, sr, ob, rb, xb, acc, hb, r2s, r2r, yb, zb, resid,
    lsem, kv_s, kv_r, wd_s, wd_r, pair_s, pair_r, r1_s, r1_r, ss_s, ss_r, a_s, a_r, ag_s, ag_r, r2_s, r2_r, b_s, b_r,
):
    s = lax.axis_index("seq")
    e = lax.axis_index("exp")
    zh = e // 2
    c = e % 2
    other = 1 - c
    pe = zh * 2 + other
    ue = lax.rem(zh + 1, 4) * 2 + c
    de = lax.rem(zh + 3, 4) * 2 + c
    fe = lax.rem(zh + 2, 4) * 2 + c

    def far(src, dst, send, recv, to_s, to_e):
        return pltpu.make_async_remote_copy(
            src_ref=src, dst_ref=dst, send_sem=send, recv_sem=recv,
            device_id={"seq": to_s, "exp": to_e}, device_id_type=MESH,
        )

    barrier = pltpu.get_barrier_semaphore()

    @pl.loop(1, NSEQ)
    def _(i):
        pl.semaphore_signal(barrier, inc=1, device_id={"seq": lax.rem(s + i, NSEQ), "exp": e}, device_id_type=MESH)

    for i in range(1, 8):
        pl.semaphore_signal(barrier, inc=1, device_id={"seq": s, "exp": lax.rem(e + i, 8)}, device_id_type=MESH)

    loads = [
        pltpu.make_async_copy(q_hbm, qs, lsem.at[0]),
        pltpu.make_async_copy(k_hbm, kb.at[0], lsem.at[1]),
        pltpu.make_async_copy(v_hbm, vb.at[0], lsem.at[2]),
        pltpu.make_async_copy(res_hbm, res, lsem.at[3]),
    ]
    w_loads = [
        pltpu.make_async_copy(
            w_hbm.at[:, pl.ds(pl.multiple_of(z * 1024 + c * COLS, COLS), COLS)], w2.at[z, c], lsem.at[4 + z])
        for z in range(4)
    ]
    e_loads = [
        pltpu.make_async_copy(gate_hbm, gu.at[pl.ds(0, UNITS)], lsem.at[8]),
        pltpu.make_async_copy(up_hbm, gu.at[pl.ds(384, UNITS)], lsem.at[9]),
    ]
    d_loads = [
        pltpu.make_async_copy(
            down_hbm.at[:, pl.ds(pl.multiple_of(z * 1024 + c * COLS, COLS), COLS)], d2.at[z, c], lsem.at[10 + z])
        for z in range(4)
    ]
    for copy in loads + w_loads + e_loads + d_loads:
        copy.start()
    gu[UNITS:384, :] = jnp.broadcast_to(router_ref[...].astype(F32), (32, D)).astype(BF16)

    pl.semaphore_wait(barrier, NSEQ - 1 + 7)

    kv = []
    for k in range(1, 5):
        to = lax.rem(s + k, NSEQ)
        kv.append([
            far(ids_ref, sb.at[k], kv_s.at[k - 1, 0], kv_r.at[k - 1, 0], to, e),
            far(k_hbm, kb.at[k], kv_s.at[k - 1, 1], kv_r.at[k - 1, 1], to, e),
            far(v_hbm, vb.at[k], kv_s.at[k - 1, 2], kv_r.at[k - 1, 2], to, e),
        ])
    for j in range(3):
        for trio in kv:
            trio[j].start()
    wd = [
        far(w_hbm.at[:, pl.ds(pl.multiple_of(z * 1024 + other * COLS, COLS), COLS)], w2.at[z, c],
            wd_s.at[z], wd_r.at[z], s, pe)
        for z in range(4)
    ] + [
        far(down_hbm.at[:, pl.ds(pl.multiple_of(z * 1024 + other * COLS, COLS), COLS)], d2.at[z, c],
            wd_s.at[4 + z], wd_r.at[4 + z], s, pe)
        for z in range(4)
    ]
    for copy in wd:
        copy.start()

    ids = ids_ref[...].astype(F32)
    seg_row, picked_row = ids[0:1, :], ids[1:2, :]
    seg_col = as_column(seg_row)
    picked_col = as_column(picked_row)
    same = picked_col == jnp.broadcast_to(picked_row, (TOK, TOK))
    sub, lane = iota((TOK, TOK), 0), iota((TOK, TOK), 1)
    rank_row = jnp.sum(jnp.where(same & (sub < lane), 1.0, 0.0), axis=0, keepdims=True)
    rank_col = jnp.sum(jnp.where(same & (lane < sub), 1.0, 0.0), axis=1, keepdims=True)
    slot_row = picked_row * 8.0 + rank_row
    slot_col = picked_col[:, 0:1] * 8.0 + rank_col
    spread = jnp.where(iota((SLOTS, TOK), 0).astype(F32) == slot_row, 1.0, 0.0).astype(BF16)
    pick = jnp.where(iota((TOK, SLOTS), 1).astype(F32) == slot_col, 1.0, 0.0).astype(BF16)

    for copy in loads:
        copy.wait()
    scores = []
    for k in range(5):
        if k == 0:
            allowed = (seg_col == seg_row) & (lane <= sub)
        else:
            kv[k - 1][0].wait_recv()
            kv[k - 1][1].wait_recv()
            shift = jnp.where(s >= k, 0.0, 1000.0)
            allowed = seg_col == sb[k][0:1, :].astype(F32) + shift
        both = []
        for h in range(2):
            cols = slice(h * HEAD, (h + 1) * HEAD)
            raw = dot_nt(qs[:, cols], kb[k, :, cols]) * HEAD ** (-0.5)
            both.append(jnp.where(allowed, raw, NEGATIVE))
        scores.append(both)
    for k in range(1, 5):
        kv[k - 1][2].wait_recv()
    for h in range(2):
        cols = slice(h * HEAD, (h + 1) * HEAD)
        top = scores[0][h]
        for k in range(1, 5):
            top = jnp.maximum(top, scores[k][h])
        top = jnp.max(top, axis=1, keepdims=True)
        total = jnp.zeros((TOK, TOK), F32)
        numer = jnp.zeros((TOK, HEAD), F32)
        for k in range(5):
            weight = jnp.exp(scores[k][h] - top)
            total = total + weight
            numer = numer + dot(weight.astype(BF16), vb[k, :, cols])
        denom = jnp.sum(total, axis=1, keepdims=True)
        att[c, :, cols] = (numer / denom).astype(BF16)
    att_x = far(att.at[c], att.at[c], pair_s.at[0], pair_r.at[0], s, pe)
    att_x.start()
    for copy in w_loads:
        copy.wait()
    for z in range(4):
        wd[z].wait_recv()
    att_x.wait_recv()

    def reduced(part, sent, came, sends, recvs):
        def go(i, to):
            copy = far(sent.at[i], came.at[i], sends.at[i], recvs.at[i], s, to)
            copy.start()
            return copy

        value = part(lax.rem(zh + 2, 4))
        sent[0] = value[:, :HALF].astype(BF16)
        sent[3] = value[:, HALF:].astype(BF16)
        c0, c3 = go(0, ue), go(3, de)
        up_value = part(lax.rem(zh + 1, 4))
        sent[1] = up_value[:, HALF:].astype(BF16)
        c1 = go(1, ue)
        down_value = part(lax.rem(zh + 3, 4))
        sent[4] = down_value[:, :HALF].astype(BF16)
        c4 = go(4, de)
        own = part(zh)
        c0.wait_recv()
        sent[2] = (up_value[:, :HALF] + came[0].astype(F32)).astype(BF16)
        c2 = go(2, ue)
        c3.wait_recv()
        sent[5] = (down_value[:, HALF:] + came[3].astype(F32)).astype(BF16)
        c5 = go(5, de)
        for copy in (c1, c4, c2, c5):
            copy.wait_recv()
        left = own[:, :HALF] + came[2].astype(F32) + came[4].astype(F32)
        right = own[:, HALF:] + came[1].astype(F32) + came[5].astype(F32)
        return left, right, (c0, c1, c2, c3, c4, c5)

    def projected(z):
        return dot(att[0], w2[z, 0]) + dot(att[1], w2[z, 1])

    left, right, r1 = reduced(projected, r1s, r1r, r1_s, r1_r)
    left = res[:, :HALF].astype(F32) + left
    right = res[:, HALF:].astype(F32) + right
    resid[:, :HALF] = left
    resid[:, HALF:] = right

    squares = jnp.sum(left * left + right * right, axis=1, keepdims=True)
    squares = jnp.transpose(jnp.broadcast_to(squares, (TOK, TOK)))[0:8, :]
    ss[...] = squares
    sr[e] = squares
    ss_x = []
    for i in range(1, 8):
        copy = far(ss, sr.at[e], ss_s.at[i - 1], ss_r.at[0], s, lax.rem(e + i, 8))
        copy.start()
        ss_x.append(copy)
    pltpu.make_async_copy(sr.at[pl.ds(0, 7)], sr.at[pl.ds(0, 7)], ss_r.at[0]).wait()
    sum_row = jnp.sum(sr[...], axis=0)[0:1, :]
    scale = as_column(lax.rsqrt(sum_row / D + EPSILON))[:, 0:1]
    normed = (resid[...] * scale * gain_ref[...]).astype(BF16)

    ob[...] = dot(spread, normed).reshape(NSEQ, 8, COLS).astype(BF16)
    rb[s] = ob[s]

    @pl.loop(1, NSEQ)
    def _(i):
        to = lax.rem(s + i, NSEQ)
        far(ob.at[to], rb.at[s], a_s.at[0], a_r.at[0], to, e).start()

    pltpu.make_async_copy(ob.at[pl.ds(0, NSEQ - 1)], rb.at[pl.ds(0, NSEQ - 1)], a_r.at[0]).wait()
    row, col = iota((ROWS, SLOTS), 0), iota((ROWS, SLOTS), 1)
    tight = jnp.where((row == (col >> 3) * 7 + (col & 7)) & ((col & 7) < 7), 1.0, 0.0).astype(BF16)
    row, col = iota((SLOTS, ROWS), 0), iota((SLOTS, ROWS), 1)
    loose = jnp.where((col == (row >> 3) * 7 + (row & 7)) & ((row & 7) < 7), 1.0, 0.0).astype(BF16)
    xb[e] = dot(tight, rb[...].astype(F32).reshape(SLOTS, COLS).astype(BF16)).astype(BF16)

    first, second = pl.ds(0, ROWS // 2), pl.ds(ROWS // 2, ROWS // 2)

    def pass_on(i, src_e, rows, to):
        return far(xb.at[src_e, rows], xb.at[src_e, rows], ag_s.at[i], ag_r.at[i], s, to)

    def share(i, src_e):
        return far(xb.at[src_e], xb.at[src_e], ag_s.at[i], ag_r.at[i], s, pe)

    g0, g2 = pass_on(0, e, first, ue), pass_on(2, e, second, de)
    g1, g3 = pass_on(1, e, second, ue), pass_on(3, e, first, de)
    g4, g5 = pass_on(4, de, first, ue), pass_on(5, ue, second, de)
    g6, g7, g8, g9 = share(6, e), share(7, de), share(8, ue), share(9, fe)
    for copy in (g0, g2, g6, g1, g3):
        copy.start()

    def absorb(src_e):
        return dot_nt(xb[src_e], gu[:, pl.ds(pl.multiple_of(src_e * COLS, COLS), COLS)])

    def flip(src_e):
        return src_e + 1 - 2 * c

    for copy in e_loads:
        copy.wait()
    acc[...] = absorb(e)
    g6.wait_recv()
    acc[...] += absorb(pe)
    g0.wait_recv()
    g4.start()
    g2.wait_recv()
    g5.start()
    g1.wait_recv()
    g7.start()
    g3.wait_recv()
    g8.start()
    acc[...] += absorb(de)
    acc[...] += absorb(ue)
    g7.wait_recv()
    acc[...] += absorb(flip(de))
    g8.wait_recv()
    acc[...] += absorb(flip(ue))
    g4.wait_recv()
    g5.wait_recv()
    g9.start()
    acc[...] += absorb(fe)
    g9.wait_recv()
    acc[...] += absorb(flip(fe))

    gate_sum = acc[:, 0:UNITS]
    up_sum = acc[:, 384:384 + UNITS]
    logit = acc[:, UNITS:UNITS + 1]
    hidden = gate_sum / (1.0 + jnp.exp(-gate_sum)) * up_sum * (1.0 / (1.0 + jnp.exp(-logit)))
    hb[c] = hidden.astype(BF16)
    hid_x = far(hb.at[c], hb.at[c], pair_s.at[1], pair_r.at[1], s, pe)
    hid_x.start()
    for copy in d_loads:
        copy.wait()
    for z in range(4, 8):
        wd[z].wait_recv()
    hid_x.wait_recv()

    def expert_out(z):
        return dot(hb[0], d2[z, 0]) + dot(hb[1], d2[z, 1])

    left, right, r2 = reduced(expert_out, r2s, r2r, r2_s, r2_r)
    yb[:, :, :HALF] = dot(loose, left.astype(BF16)).reshape(NSEQ, 8, HALF).astype(BF16)
    yb[:, :, HALF:] = dot(loose, right.astype(BF16)).reshape(NSEQ, 8, HALF).astype(BF16)
    zb[s] = yb[s]

    @pl.loop(1, NSEQ)
    def _(i):
        to = lax.rem(s + i, NSEQ)
        far(yb.at[to], zb.at[s], b_s.at[0], b_r.at[0], to, e).start()

    pltpu.make_async_copy(yb.at[pl.ds(0, NSEQ - 1)], zb.at[pl.ds(0, NSEQ - 1)], b_r.at[0]).wait()
    routed = dot(pick, zb[...].astype(F32).reshape(SLOTS, COLS).astype(BF16))
    out_ref[...] = (resid[...] + routed).astype(BF16)

    for trio in kv:
        for copy in trio:
            copy.wait_send()
    for copy in wd + [att_x, hid_x, *r1, *r2, *ss_x, g0, g1, g2, g3, g4, g5, g6, g7, g8, g9]:
        copy.wait_send()
    for buf, sem in ((ob, a_s), (yb, b_s)):
        pltpu.make_async_copy(buf.at[pl.ds(0, NSEQ - 1)], buf.at[pl.ds(0, NSEQ - 1)], sem.at[0]).wait()


def local(
    query_input, key_input, value_input, segment_ids, residual_in, out_weight, norm_gain, router,
    modality, expert_in, gate_weight, up_weight, down_weight,
):
    ids = jnp.concatenate([
        segment_ids[None], (modality * 16 + expert_in)[None], jnp.zeros((6, TOK), jnp.int32)
    ])
    anywhere = pl.BlockSpec(memory_space=pl.ANY)
    vmem = pl.BlockSpec(memory_space=pltpu.VMEM)
    V = pltpu.VMEM
    dma = pltpu.SemaphoreType.DMA
    return pl.pallas_call(
        kernel,
        out_shape=jax.ShapeDtypeStruct((TOK, COLS), BF16),
        in_specs=[anywhere, anywhere, anywhere, vmem, anywhere, anywhere, vmem, vmem, anywhere, anywhere, anywhere],
        out_specs=vmem,
        scratch_shapes=[
            V((TOK, WIDE), BF16),
            V((5, TOK, WIDE), BF16),
            V((5, TOK, WIDE), BF16),
            V((5, 8, TOK), jnp.int32),
            V((TOK, COLS), BF16),
            V((4, 2, WIDE, COLS), BF16),
            V((736, D), BF16),
            V((4, 2, UNITS, COLS), BF16),
            V((2, TOK, WIDE), BF16),
            V((6, TOK, HALF), BF16),
            V((6, TOK, HALF), BF16),
            V((8, TOK), F32),
            V((8, 8, TOK), F32),
            V((NSEQ, 8, COLS), BF16),
            V((NSEQ, 8, COLS), BF16),
            V((8, ROWS, COLS), BF16),
            V((ROWS, 736), F32),
            V((2, ROWS, UNITS), BF16),
            V((6, ROWS, HALF), BF16),
            V((6, ROWS, HALF), BF16),
            V((NSEQ, 8, COLS), BF16),
            V((NSEQ, 8, COLS), BF16),
            V((TOK, COLS), F32),
            dma((14,)),
            dma((4, 3)), dma((4, 3)),
            dma((8,)), dma((8,)),
            dma((2,)), dma((2,)),
            dma((6,)), dma((6,)),
            dma((7,)), dma((1,)),
            dma((1,)), dma((1,)),
            dma((10,)), dma((10,)),
            dma((6,)), dma((6,)),
            dma((1,)), dma((1,)),
        ],
        compiler_params=pltpu.CompilerParams(
            collective_id=0, has_side_effects=True, vmem_limit_bytes=60 * 1024 * 1024),
    )(
        query_input, key_input, value_input, ids, residual_in, out_weight, norm_gain.reshape(1, COLS),
        router.T, gate_weight[0].T, up_weight[0].T, down_weight[0],
    )


def solution(mesh):
    placed = (
        P("seq", "exp"), P("seq", "exp"), P("seq", "exp"), P("seq"), P("seq", "exp"), P("exp", None), P("exp"),
        P(None, "seq"), P("seq"), P("seq"), P("seq", None, "exp"), P("seq", None, "exp"), P("seq", "exp", None),
    )
    return jax.shard_map(local, mesh=mesh, in_specs=placed, out_specs=P("seq", "exp"), check_vma=False)
```

```python
import jax
import jax.numpy as jnp
from jax import lax
from jax.experimental import pallas as pl
from jax.experimental.pallas import tpu as pltpu
from jax.sharding import PartitionSpec as P

D = 4096
EPSILON = 1e-05
NEGATIVE = -1e30
TOK = 128
HEAD = 128
WIDE = 256
COLS = 512
HALF = 256
NSEQ = 32
ROWS = 224
SLOTS = 256
UNITS = 352
MESH = pl.DeviceIdType.MESH
F32 = jnp.float32
BF16 = jnp.bfloat16


def dot(a, b):
    return jnp.dot(a, b, preferred_element_type=F32)


def dot_nt(a, b):
    return lax.dot_general(a, b, (((1,), (1,)), ((), ())), preferred_element_type=F32)


def iota(shape, dim):
    return lax.broadcasted_iota(jnp.int32, shape, dim)


def as_column(row):
    return jnp.transpose(jnp.broadcast_to(row, (TOK, TOK)))


def kernel(
    q_hbm, k_hbm, v_hbm, seg_hbm, mod_hbm, pick_hbm, res_hbm, w_hbm, gain_hbm, router_hbm, gate_hbm, up_hbm, down_hbm,
    out_ref,
    qs, kb, vb, sb, mods, picks, gains, rout, res, w2, gu, d2, att, r1s, r1r, ss, sr, ob, rb, osc, rsc, xb, acc, hb,
    r2s, r2r, yb, zb, resid, known, lsem, kv_s, kv_r, wd_s, wd_r, pair_s, pair_r, r1_s, r1_r, ss_s, ss_r, a_s, a_r, c_s, c_r, ag_s, ag_r, r2_s, r2_r, b_s, b_r,
):
    s = lax.axis_index("seq")
    e = lax.axis_index("exp")
    zh = e // 2
    c = e % 2
    other = 1 - c
    pe = zh * 2 + other
    ue = lax.rem(zh + 1, 4) * 2 + c
    de = lax.rem(zh + 3, 4) * 2 + c
    fe = lax.rem(zh + 2, 4) * 2 + c

    def far(src, dst, send, recv, to_s, to_e):
        return pltpu.make_async_remote_copy(
            src_ref=src, dst_ref=dst, send_sem=send, recv_sem=recv,
            device_id={"seq": to_s, "exp": to_e}, device_id_type=MESH,
        )

    def ring(i):
        return lax.rem(s + i + NSEQ, NSEQ)

    def tell(sem, to_s, to_e):
        pl.semaphore_signal(sem, inc=1, device_id={"seq": to_s, "exp": to_e}, device_id_type=MESH)

    barrier = pltpu.get_barrier_semaphore()
    for i in (1, 2, 3, 4, -1, -2, -3, -4):
        tell(barrier, ring(i), e)
    for to in (pe, ue, de):
        tell(barrier, s, to)

    loads = [
        pltpu.make_async_copy(q_hbm, qs, lsem.at[0]),
        pltpu.make_async_copy(k_hbm, kb.at[0], lsem.at[1]),
        pltpu.make_async_copy(v_hbm, vb.at[0], lsem.at[2]),
        pltpu.make_async_copy(seg_hbm, sb.at[0], lsem.at[14]),
    ]
    later = [
        pltpu.make_async_copy(mod_hbm, mods, lsem.at[15]),
        pltpu.make_async_copy(pick_hbm, picks, lsem.at[16]),
        pltpu.make_async_copy(gain_hbm, gains, lsem.at[17]),
        pltpu.make_async_copy(router_hbm, rout, lsem.at[18]),
        pltpu.make_async_copy(res_hbm, res, lsem.at[3]),
    ]
    w_loads = [
        pltpu.make_async_copy(
            w_hbm.at[:, pl.ds(pl.multiple_of(z * 1024 + c * COLS, COLS), COLS)], w2.at[z, c], lsem.at[4 + z])
        for z in range(4)
    ]
    e_loads = [
        pltpu.make_async_copy(gate_hbm, gu.at[pl.ds(0, UNITS)], lsem.at[8]),
        pltpu.make_async_copy(up_hbm, gu.at[pl.ds(384, UNITS)], lsem.at[9]),
    ]
    d_loads = [
        pltpu.make_async_copy(
            down_hbm.at[:, pl.ds(pl.multiple_of(z * 1024 + c * COLS, COLS), COLS)], d2.at[z, c], lsem.at[10 + z])
        for z in range(4)
    ]
    for copy in loads + later + w_loads + e_loads + d_loads:
        copy.start()
    for copy in loads:
        copy.wait()
    pl.semaphore_wait(barrier, 11)

    kv = []
    for k in range(1, 5):
        to = ring(k)
        kv.append([
            far(sb.at[0], sb.at[k], kv_s.at[k - 1, 0], kv_r.at[k - 1, 0], to, e),
            far(kb.at[0], kb.at[k], kv_s.at[k - 1, 1], kv_r.at[k - 1, 1], to, e),
            far(vb.at[0], vb.at[k], kv_s.at[k - 1, 2], kv_r.at[k - 1, 2], to, e),
        ])
    for j in range(3):
        for trio in kv:
            trio[j].start()
    wd = [
        far(w_hbm.at[:, pl.ds(pl.multiple_of(z * 1024 + other * COLS, COLS), COLS)], w2.at[z, c],
            wd_s.at[z], wd_r.at[z], s, pe)
        for z in range(4)
    ] + [
        far(down_hbm.at[:, pl.ds(pl.multiple_of(z * 1024 + other * COLS, COLS), COLS)], d2.at[z, c],
            wd_s.at[4 + z], wd_r.at[4 + z], s, pe)
        for z in range(4)
    ]
    tell(known.at[0], ring(4), e)
    tell(known.at[0], ring(-4), e)
    for copy in wd:
        copy.start()

    for copy in later:
        copy.wait()
    gu[UNITS:384, :] = jnp.broadcast_to(rout[...].astype(F32), (32, D)).astype(BF16)
    seg_row, picked_row = sb[0].astype(F32), (mods[...] * 16 + picks[...]).astype(F32)
    seg_col = as_column(seg_row)
    picked_col = as_column(picked_row)
    same = picked_col == jnp.broadcast_to(picked_row, (TOK, TOK))
    sub, lane = iota((TOK, TOK), 0), iota((TOK, TOK), 1)
    rank_row = jnp.sum(jnp.where(same & (sub < lane), 1.0, 0.0), axis=0, keepdims=True)
    rank_col = jnp.sum(jnp.where(same & (lane < sub), 1.0, 0.0), axis=1, keepdims=True)
    slot_row = picked_row * 8.0 + rank_row
    slot_col = picked_col[:, 0:1] * 8.0 + rank_col
    spread = jnp.where(iota((SLOTS, TOK), 0).astype(F32) == slot_row, 1.0, 0.0).astype(BF16)
    pick = jnp.where(iota((TOK, SLOTS), 1).astype(F32) == slot_col, 1.0, 0.0).astype(BF16)

    pl.semaphore_wait(known.at[0], 2)
    tell(known.at[1], ring(8), e)
    tell(known.at[1], ring(-8), e)

    scores = []
    for k in range(5):
        if k == 0:
            allowed = (seg_col == seg_row) & (lane <= sub)
        else:
            kv[k - 1][0].wait_recv()
            kv[k - 1][1].wait_recv()
            shift = jnp.where(s >= k, 0.0, 1000.0)
            allowed = seg_col == sb[k].astype(F32) + shift
        both = []
        for h in range(2):
            cols = slice(h * HEAD, (h + 1) * HEAD)
            raw = dot_nt(qs[:, cols], kb[k, :, cols]) * HEAD ** (-0.5)
            both.append(jnp.where(allowed, raw, NEGATIVE))
        scores.append(both)
    for k in range(1, 5):
        kv[k - 1][2].wait_recv()
    for h in range(2):
        cols = slice(h * HEAD, (h + 1) * HEAD)
        top = scores[0][h]
        for k in range(1, 5):
            top = jnp.maximum(top, scores[k][h])
        top = jnp.max(top, axis=1, keepdims=True)
        total = jnp.zeros((TOK, TOK), F32)
        numer = jnp.zeros((TOK, HEAD), F32)
        for k in range(5):
            weight = jnp.exp(scores[k][h] - top)
            total = total + weight
            numer = numer + dot(weight.astype(BF16), vb[k, :, cols])
        denom = jnp.sum(total, axis=1, keepdims=True)
        att[c, :, cols] = (numer / denom).astype(BF16)
    att_x = far(att.at[c], att.at[c], pair_s.at[0], pair_r.at[0], s, pe)
    att_x.start()
    for copy in w_loads:
        copy.wait()
    for z in range(4):
        wd[z].wait_recv()
    att_x.wait_recv()

    def reduced(part, sent, came, sends, recvs):
        def go(i, to):
            copy = far(sent.at[i], came.at[i], sends.at[i], recvs.at[i], s, to)
            copy.start()
            return copy

        value = part(lax.rem(zh + 2, 4))
        sent[0] = value[:, :HALF].astype(BF16)
        sent[3] = value[:, HALF:].astype(BF16)
        c0, c3 = go(0, ue), go(3, de)
        up_value = part(lax.rem(zh + 1, 4))
        sent[1] = up_value[:, HALF:].astype(BF16)
        c1 = go(1, ue)
        down_value = part(lax.rem(zh + 3, 4))
        sent[4] = down_value[:, :HALF].astype(BF16)
        c4 = go(4, de)
        own = part(zh)
        c0.wait_recv()
        sent[2] = (up_value[:, :HALF] + came[0].astype(F32)).astype(BF16)
        c2 = go(2, ue)
        c3.wait_recv()
        sent[5] = (down_value[:, HALF:] + came[3].astype(F32)).astype(BF16)
        c5 = go(5, de)
        for copy in (c1, c4, c2, c5):
            copy.wait_recv()
        left = own[:, :HALF] + came[2].astype(F32) + came[4].astype(F32)
        right = own[:, HALF:] + came[1].astype(F32) + came[5].astype(F32)
        return left, right, (c0, c1, c2, c3, c4, c5)

    def projected(z):
        return dot(att[0], w2[z, 0]) + dot(att[1], w2[z, 1])

    left, right, r1 = reduced(projected, r1s, r1r, r1_s, r1_r)
    left = res[:, :HALF].astype(F32) + left
    right = res[:, HALF:].astype(F32) + right
    resid[:, :HALF] = left
    resid[:, HALF:] = right

    pl.semaphore_wait(known.at[1], 2)

    gained = (resid[...] * gains[...]).astype(BF16)
    ob[...] = dot(spread, gained).reshape(NSEQ, 8, COLS).astype(BF16)

    @pl.loop(1, NSEQ)
    def _(i):
        to = lax.rem(s + i, NSEQ)
        far(ob.at[to], rb.at[s], a_s.at[0], a_r.at[0], to, e).start()

    rb[s] = ob[s]

    squares = jnp.sum(left * left + right * right, axis=1, keepdims=True)
    squares = jnp.transpose(jnp.broadcast_to(squares, (TOK, TOK)))[0:8, :]
    ss[0] = squares
    ss_p = far(ss.at[0], sr.at[0], ss_s.at[0], ss_r.at[0], s, pe)
    ss_p.start()
    ss_p.wait_recv()
    squares = squares + sr[0]
    ss[1] = squares
    ss_z = [far(ss.at[1], sr.at[i], ss_s.at[i], ss_r.at[i], s, to) for i, to in ((1, ue), (2, de), (3, fe))]
    for copy in ss_z:
        copy.start()

    pltpu.make_async_copy(ob.at[pl.ds(0, NSEQ - 1)], rb.at[pl.ds(0, NSEQ - 1)], a_r.at[0]).wait()
    row, col = iota((ROWS, SLOTS), 0), iota((ROWS, SLOTS), 1)
    tight = jnp.where((row == (col >> 3) * 7 + (col & 7)) & ((col & 7) < 7), 1.0, 0.0).astype(BF16)
    row, col = iota((SLOTS, ROWS), 0), iota((SLOTS, ROWS), 1)
    loose = jnp.where((col == (row >> 3) * 7 + (row & 7)) & ((row & 7) < 7), 1.0, 0.0).astype(BF16)
    xb[e] = dot(tight, rb[...].astype(F32).reshape(SLOTS, COLS).astype(BF16)).astype(BF16)

    first, second = pl.ds(0, ROWS // 2), pl.ds(ROWS // 2, ROWS // 2)

    def pass_on(i, src_e, rows, to):
        return far(xb.at[src_e, rows], xb.at[src_e, rows], ag_s.at[i], ag_r.at[i], s, to)

    def share(i, src_e):
        return far(xb.at[src_e], xb.at[src_e], ag_s.at[i], ag_r.at[i], s, pe)

    g0, g2 = pass_on(0, e, first, ue), pass_on(2, e, second, de)
    g1, g3 = pass_on(1, e, second, ue), pass_on(3, e, first, de)
    g4, g5 = pass_on(4, de, first, ue), pass_on(5, ue, second, de)
    g6, g7, g8, g9 = share(6, e), share(7, de), share(8, ue), share(9, fe)
    for copy in (g0, g2, g6, g1, g3):
        copy.start()

    for copy in ss_z:
        copy.wait_recv()
    scale_row = lax.rsqrt((squares + sr[1] + sr[2] + sr[3])[0:1, :] / D + EPSILON)
    slot_scale = jnp.sum(spread.astype(F32) * scale_row, axis=1, keepdims=True)
    osc[...] = jnp.broadcast_to(slot_scale, (SLOTS, TOK)).reshape(NSEQ, 8, TOK)

    @pl.loop(1, NSEQ)
    def _(i):
        to = lax.rem(s + i, NSEQ)
        far(osc.at[to], rsc.at[s], c_s.at[0], c_r.at[0], to, e).start()

    rsc[s] = osc[s]

    def absorb(src_e):
        return dot_nt(xb[src_e], gu[:, pl.ds(pl.multiple_of(src_e * COLS, COLS), COLS)])

    def flip(src_e):
        return src_e + 1 - 2 * c

    for copy in e_loads:
        copy.wait()
    acc[...] = absorb(e)
    g6.wait_recv()
    acc[...] += absorb(pe)
    g0.wait_recv()
    g4.start()
    g2.wait_recv()
    g5.start()
    g1.wait_recv()
    g7.start()
    g3.wait_recv()
    g8.start()
    acc[...] += absorb(de)
    acc[...] += absorb(ue)
    g7.wait_recv()
    acc[...] += absorb(flip(de))
    g8.wait_recv()
    acc[...] += absorb(flip(ue))
    g4.wait_recv()
    g5.wait_recv()
    g9.start()
    acc[...] += absorb(fe)
    g9.wait_recv()
    acc[...] += absorb(flip(fe))

    pltpu.make_async_copy(osc.at[pl.ds(0, NSEQ - 1)], rsc.at[pl.ds(0, NSEQ - 1)], c_r.at[0]).wait()
    scale = lax.dot_general(
        tight.astype(F32), rsc[...].reshape(SLOTS, TOK), (((1,), (0,)), ((), ())),
        precision=lax.Precision.HIGHEST, preferred_element_type=F32)[:, 0:1]
    gate_sum = acc[:, 0:UNITS] * scale
    up_sum = acc[:, 384:384 + UNITS] * scale
    logit = acc[:, UNITS:UNITS + 1] * scale
    hidden = gate_sum / (1.0 + jnp.exp(-gate_sum)) * up_sum * (1.0 / (1.0 + jnp.exp(-logit)))
    hb[c] = hidden.astype(BF16)
    hid_x = far(hb.at[c], hb.at[c], pair_s.at[1], pair_r.at[1], s, pe)
    hid_x.start()
    for copy in d_loads:
        copy.wait()
    for z in range(4, 8):
        wd[z].wait_recv()
    hid_x.wait_recv()

    def expert_out(z):
        return dot(hb[0], d2[z, 0]) + dot(hb[1], d2[z, 1])

    left, right, r2 = reduced(expert_out, r2s, r2r, r2_s, r2_r)
    yb[:, :, :HALF] = dot(loose, left.astype(BF16)).reshape(NSEQ, 8, HALF).astype(BF16)
    yb[:, :, HALF:] = dot(loose, right.astype(BF16)).reshape(NSEQ, 8, HALF).astype(BF16)
    zb[s] = yb[s]

    @pl.loop(1, NSEQ)
    def _(i):
        to = lax.rem(s + i, NSEQ)
        far(yb.at[to], zb.at[s], b_s.at[0], b_r.at[0], to, e).start()

    pltpu.make_async_copy(yb.at[pl.ds(0, NSEQ - 1)], zb.at[pl.ds(0, NSEQ - 1)], b_r.at[0]).wait()
    routed = dot(pick, zb[...].astype(F32).reshape(SLOTS, COLS).astype(BF16))
    out_ref[...] = resid[...] + routed

    for trio in kv:
        for copy in trio:
            copy.wait_send()
    for copy in wd + [att_x, hid_x, *r1, *r2, ss_p, *ss_z, g0, g1, g2, g3, g4, g5, g6, g7, g8, g9]:
        copy.wait_send()
    for buf, sem in ((ob, a_s), (osc, c_s), (yb, b_s)):
        pltpu.make_async_copy(buf.at[pl.ds(0, NSEQ - 1)], buf.at[pl.ds(0, NSEQ - 1)], sem.at[0]).wait()


def local(
    query_input, key_input, value_input, segment_ids, residual_in, out_weight, norm_gain, router,
    modality, expert_in, gate_weight, up_weight, down_weight,
):
    anywhere = pl.BlockSpec(memory_space=pltpu.HBM)
    vmem = pl.BlockSpec(memory_space=pltpu.VMEM)
    V = pltpu.VMEM
    dma = pltpu.SemaphoreType.DMA
    total = pl.pallas_call(
        kernel,
        out_shape=pltpu.VMEM((TOK, COLS), F32),
        in_specs=[anywhere] * 13,
        out_specs=vmem,
        scratch_shapes=[
            V((TOK, WIDE), BF16),
            V((5, TOK, WIDE), BF16),
            V((5, TOK, WIDE), BF16),
            V((5, 1, TOK), jnp.int32),
            V((1, TOK), jnp.int32),
            V((1, TOK), jnp.int32),
            V((1, COLS), F32),
            V((1, D), BF16),
            V((TOK, COLS), BF16),
            V((4, 2, WIDE, COLS), BF16),
            V((736, D), BF16),
            V((4, 2, UNITS, COLS), BF16),
            V((2, TOK, WIDE), BF16),
            V((6, TOK, HALF), BF16),
            V((6, TOK, HALF), BF16),
            V((2, 8, TOK), F32),
            V((4, 8, TOK), F32),
            V((NSEQ, 8, COLS), BF16),
            V((NSEQ, 8, COLS), BF16),
            V((NSEQ, 8, TOK), F32),
            V((NSEQ, 8, TOK), F32),
            V((8, ROWS, COLS), BF16),
            V((ROWS, 736), F32),
            V((2, ROWS, UNITS), BF16),
            V((6, ROWS, HALF), BF16),
            V((6, ROWS, HALF), BF16),
            V((NSEQ, 8, COLS), BF16),
            V((NSEQ, 8, COLS), BF16),
            V((TOK, COLS), F32),
            pltpu.SemaphoreType.REGULAR((2,)),
            dma((19,)),
            dma((4, 3)), dma((4, 3)),
            dma((8,)), dma((8,)),
            dma((2,)), dma((2,)),
            dma((6,)), dma((6,)),
            dma((4,)), dma((4,)),
            dma((1,)), dma((1,)),
            dma((1,)), dma((1,)),
            dma((10,)), dma((10,)),
            dma((6,)), dma((6,)),
            dma((1,)), dma((1,)),
        ],
        compiler_params=pltpu.CompilerParams(
            collective_id=0, has_side_effects=True, vmem_limit_bytes=67043328 - 278528),
    )(
        query_input, key_input, value_input, segment_ids.reshape(1, TOK), modality.reshape(1, TOK),
        expert_in.reshape(1, TOK), residual_in, out_weight, norm_gain.reshape(1, COLS),
        router.T, gate_weight[0].T, up_weight[0].T, down_weight[0],
    )
    return total.astype(BF16)


def solution(mesh):
    placed = (
        P("seq", "exp"), P("seq", "exp"), P("seq", "exp"), P("seq"), P("seq", "exp"), P("exp", None), P("exp"),
        P(None, "seq"), P("seq"), P("seq"), P("seq", None, "exp"), P("seq", None, "exp"), P("seq", "exp", None),
    )
    return jax.shard_map(local, mesh=mesh, in_specs=placed, out_specs=P("seq", "exp"), check_vma=False)
```

```python
import jax
import jax.numpy as jnp
from jax import lax
from jax.experimental import pallas as pl
from jax.experimental.pallas import tpu as pltpu
from jax.sharding import PartitionSpec as P

D = 4096
EPSILON = 1e-05
NEGATIVE = -1e30
TOK = 128
HEAD = 128
WIDE = 256
COLS = 512
HALF = 256
QUART = 128
NSEQ = 32
ROWS = 224
SLOTS = 256
UNITS = 352
MESH = pl.DeviceIdType.MESH
F32 = jnp.float32
BF16 = jnp.bfloat16


def dot(a, b):
    return jnp.dot(a, b, preferred_element_type=F32)


def dot_nt(a, b):
    return lax.dot_general(a, b, (((1,), (1,)), ((), ())), preferred_element_type=F32)


def exact_dot(a, b):
    return jnp.dot(a, b, precision=lax.Precision.HIGHEST, preferred_element_type=F32)


def iota(shape, dim):
    return lax.broadcasted_iota(jnp.int32, shape, dim)


def as_column(row):
    return jnp.transpose(jnp.broadcast_to(row, (TOK, TOK)))


def kernel(
    q_hbm, k_hbm, v_hbm, seg_hbm, mod_hbm, pick_hbm, res_hbm, w_hbm, gain_hbm, router_hbm, gate_hbm, up_hbm, down_hbm,
    out_ref,
    qs, kb, vb, sb, mods, picks, gains, rout, res, w2, gu, d2, att, r1s, r1r, ss, sr, ob, rb, osc, rsc, xb, acc, hb,
    r2s, r2r, yb, zb, resid, known, lsem, kv_s, kv_r, wd_s, wd_r, pair_s, pair_r, r1_s, r1_r, ss_s, ss_r, a_s, a_r, c_s, c_r, ag_s, ag_r, r2_s, r2_r, b_s, b_r,
):
    s = lax.axis_index("seq")
    e = lax.axis_index("exp")
    zh = e // 2
    c = e % 2
    other = 1 - c
    pe = zh * 2 + other
    ue = lax.rem(zh + 1, 4) * 2 + c
    de = lax.rem(zh + 3, 4) * 2 + c
    fe = lax.rem(zh + 2, 4) * 2 + c
    pfe = lax.rem(zh + 2, 4) * 2 + other

    def far(src, dst, send, recv, to_s, to_e):
        return pltpu.make_async_remote_copy(
            src_ref=src, dst_ref=dst, send_sem=send, recv_sem=recv,
            device_id={"seq": to_s, "exp": to_e}, device_id_type=MESH,
        )

    def ring(i):
        return lax.rem(s + i + NSEQ, NSEQ)

    def tell(sem, to_s, to_e):
        pl.semaphore_signal(sem, inc=1, device_id={"seq": to_s, "exp": to_e}, device_id_type=MESH)

    barrier = pltpu.get_barrier_semaphore()
    for i in (1, 2, 3, 4, -1, -2, -3, -4):
        tell(barrier, ring(i), e)
    for to in (pe, ue, de):
        tell(barrier, s, to)

    loads = [
        pltpu.make_async_copy(q_hbm, qs, lsem.at[0]),
        pltpu.make_async_copy(k_hbm, kb.at[0], lsem.at[1]),
        pltpu.make_async_copy(v_hbm, vb.at[0], lsem.at[2]),
        pltpu.make_async_copy(seg_hbm, sb.at[0], lsem.at[14]),
    ]
    later = [
        pltpu.make_async_copy(mod_hbm, mods, lsem.at[15]),
        pltpu.make_async_copy(pick_hbm, picks, lsem.at[16]),
        pltpu.make_async_copy(gain_hbm, gains, lsem.at[17]),
        pltpu.make_async_copy(router_hbm, rout, lsem.at[18]),
        pltpu.make_async_copy(res_hbm, res, lsem.at[3]),
    ]
    w_loads = [
        pltpu.make_async_copy(
            w_hbm.at[:, pl.ds(pl.multiple_of(z * 1024 + c * COLS, COLS), COLS)], w2.at[z, c], lsem.at[4 + z])
        for z in range(4)
    ]
    e_loads = [
        pltpu.make_async_copy(gate_hbm, gu.at[pl.ds(0, UNITS)], lsem.at[8]),
        pltpu.make_async_copy(up_hbm, gu.at[pl.ds(384, UNITS)], lsem.at[9]),
    ]
    d_loads = [
        pltpu.make_async_copy(
            down_hbm.at[:, pl.ds(pl.multiple_of(z * 1024 + c * COLS, COLS), COLS)], d2.at[z, c], lsem.at[10 + z])
        for z in range(4)
    ]
    for copy in loads + later + w_loads + e_loads + d_loads:
        copy.start()
    for copy in loads:
        copy.wait()
    pl.semaphore_wait(barrier, 11)

    last = lax.rem(s, 4) == 3

    def trio_of(k, src, to):
        return [
            far(buf.at[src], buf.at[k], kv_s.at[k - 1, j], kv_r.at[k - 1, j], to, e)
            for j, buf in enumerate((sb, kb, vb))
        ]

    kv = [trio_of(k, 0, ring(k)) for k in range(1, 5)]
    relay = trio_of(1, 4, ring(-3))
    for k in (4, 3, 2):
        kv[k - 1][0].start()
    for k in (4, 3, 2):
        kv[k - 1][1].start()
        kv[k - 1][2].start()

    @pl.when(jnp.logical_not(last))
    def _():
        for copy in kv[0]:
            copy.start()

    wd = [
        far(w_hbm.at[:, pl.ds(pl.multiple_of(z * 1024 + other * COLS, COLS), COLS)], w2.at[z, c],
            wd_s.at[z], wd_r.at[z], s, pe)
        for z in range(4)
    ] + [
        far(down_hbm.at[:, pl.ds(pl.multiple_of(z * 1024 + other * COLS, COLS), COLS)], d2.at[z, c],
            wd_s.at[4 + z], wd_r.at[4 + z], s, pe)
        for z in range(4)
    ]
    tell(known.at[0], ring(4), e)
    tell(known.at[0], ring(-4), e)
    for copy in wd:
        copy.start()

    for copy in later:
        copy.wait()
    gu[UNITS:384, :] = jnp.broadcast_to(rout[...].astype(F32), (32, D)).astype(BF16)
    seg_row, picked_row = sb[0].astype(F32), (mods[...] * 16 + picks[...]).astype(F32)
    seg_col = as_column(seg_row)
    picked_col = as_column(picked_row)
    same = picked_col == jnp.broadcast_to(picked_row, (TOK, TOK))
    sub, lane = iota((TOK, TOK), 0), iota((TOK, TOK), 1)
    rank_row = jnp.sum(jnp.where(same & (sub < lane), 1.0, 0.0), axis=0, keepdims=True)
    rank_col = jnp.sum(jnp.where(same & (lane < sub), 1.0, 0.0), axis=1, keepdims=True)
    slot_row = picked_row * 8.0 + rank_row
    slot_col = picked_col[:, 0:1] * 8.0 + rank_col
    spread = jnp.where(iota((SLOTS, TOK), 0).astype(F32) == slot_row, 1.0, 0.0).astype(BF16)
    pick = jnp.where(iota((TOK, SLOTS), 1).astype(F32) == slot_col, 1.0, 0.0).astype(BF16)

    for copy in kv[3]:
        copy.wait_recv()

    @pl.when(last)
    def _():
        for copy in relay:
            copy.start()

    pl.semaphore_wait(known.at[0], 2)
    tell(known.at[1], ring(8), e)
    tell(known.at[1], ring(-8), e)

    scores = [None] * 5
    for k in (0, 4, 3, 2, 1):
        if k == 0:
            allowed = (seg_col == seg_row) & (lane <= sub)
        else:
            if k < 4:
                for copy in kv[k - 1]:
                    copy.wait_recv()
            shift = jnp.where(s >= k, 0.0, 1000.0)
            allowed = seg_col == sb[k].astype(F32) + shift
        both = []
        for h in range(2):
            cols = slice(h * HEAD, (h + 1) * HEAD)
            raw = dot_nt(qs[:, cols], kb[k, :, cols]) * HEAD ** (-0.5)
            both.append(jnp.where(allowed, raw, NEGATIVE))
        scores[k] = both
    for h in range(2):
        cols = slice(h * HEAD, (h + 1) * HEAD)
        top = scores[0][h]
        for k in range(1, 5):
            top = jnp.maximum(top, scores[k][h])
        top = jnp.max(top, axis=1, keepdims=True)
        total = jnp.zeros((TOK, TOK), F32)
        numer = jnp.zeros((TOK, HEAD), F32)
        for k in range(5):
            weight = jnp.exp(scores[k][h] - top)
            total = total + weight
            numer = numer + dot(weight.astype(BF16), vb[k, :, cols])
        denom = jnp.sum(total, axis=1, keepdims=True)
        att[c, :, cols] = (numer / denom).astype(BF16)
    att_x = far(att.at[c], att.at[c], pair_s.at[0], pair_r.at[0], s, pe)
    att_x.start()
    for copy in w_loads:
        copy.wait()
    for z in range(4):
        wd[z].wait_recv()
    att_x.wait_recv()

    def reduced(part, sent, came, sends, recvs, emit):
        copies = []

        def go(f, i, to):
            copy = far(sent.at[f, i], came.at[f, i], sends.at[f, i], recvs.at[f, i], s, to)
            copy.start()
            copies.append(copy)
            return copy

        ahead = []
        for f in range(2):
            value = part(lax.rem(zh + 2, 4), f)
            sent[f, 0] = value[:, :QUART].astype(BF16)
            sent[f, 3] = value[:, QUART:].astype(BF16)
            ahead.append((go(f, 0, ue), go(f, 3, de)))
        waits, owns = [], []
        for f in range(2):
            up_value = part(lax.rem(zh + 1, 4), f)
            sent[f, 1] = up_value[:, QUART:].astype(BF16)
            c1 = go(f, 1, ue)
            down_value = part(lax.rem(zh + 3, 4), f)
            sent[f, 4] = down_value[:, :QUART].astype(BF16)
            c4 = go(f, 4, de)
            owns.append(part(zh, f))
            ahead[f][0].wait_recv()
            sent[f, 2] = (up_value[:, :QUART] + came[f, 0].astype(F32)).astype(BF16)
            c2 = go(f, 2, ue)
            ahead[f][1].wait_recv()
            sent[f, 5] = (down_value[:, QUART:] + came[f, 3].astype(F32)).astype(BF16)
            c5 = go(f, 5, de)
            waits.append((c1, c4, c2, c5))
        for f in range(2):
            for copy in waits[f]:
                copy.wait_recv()
            left = owns[f][:, :QUART] + came[f, 2].astype(F32) + came[f, 4].astype(F32)
            right = owns[f][:, QUART:] + came[f, 1].astype(F32) + came[f, 5].astype(F32)
            emit(f, left, right)
        return copies

    def scatter(outs, ins, send, recv):
        @pl.loop(1, NSEQ)
        def _(i):
            to = lax.rem(s + i, NSEQ)
            far(outs.at[to], ins.at[s], send, recv, to, e).start()

        ins[s] = outs[s]

    def arrive(outs, ins, sem):
        pltpu.make_async_copy(outs.at[pl.ds(0, NSEQ - 1)], ins.at[pl.ds(0, NSEQ - 1)], sem).wait()

    def projected(z, f):
        cols = slice(f * HALF, (f + 1) * HALF)
        return dot(att[0], w2[z, 0, :, cols]) + dot(att[1], w2[z, 1, :, cols])

    partial_squares = []

    def to_experts(f, left, right):
        low, high = slice(f * HALF, f * HALF + QUART), slice(f * HALF + QUART, (f + 1) * HALF)
        left = res[:, low].astype(F32) + left
        right = res[:, high].astype(F32) + right
        resid[:, low] = left
        resid[:, high] = right
        partial_squares.append(left * left + right * right)
        gained = (resid[:, f * HALF:(f + 1) * HALF] * gains[:, f * HALF:(f + 1) * HALF]).astype(BF16)
        ob[f] = dot(spread, gained).reshape(NSEQ, 8, HALF).astype(BF16)
        scatter(ob.at[f], rb.at[f], a_s.at[f], a_r.at[f])

    pl.semaphore_wait(known.at[1], 2)
    r1 = reduced(projected, r1s, r1r, r1_s, r1_r, to_experts)

    squares = jnp.sum(partial_squares[0] + partial_squares[1], axis=1, keepdims=True)
    squares = jnp.transpose(jnp.broadcast_to(squares, (TOK, TOK)))[0:8, :]
    ss[0] = squares
    ss_p = far(ss.at[0], sr.at[0], ss_s.at[0], ss_r.at[0], s, pe)
    ss_p.start()

    row, col = iota((ROWS, SLOTS), 0), iota((ROWS, SLOTS), 1)
    tight = jnp.where((row == (col >> 3) * 7 + (col & 7)) & ((col & 7) < 7), 1.0, 0.0).astype(BF16)
    row, col = iota((SLOTS, ROWS), 0), iota((SLOTS, ROWS), 1)
    loose = jnp.where((col == (row >> 3) * 7 + (row & 7)) & ((row & 7) < 7), 1.0, 0.0).astype(BF16)

    first, second = pl.ds(0, ROWS // 2), pl.ds(ROWS // 2, ROWS // 2)
    every = pl.ds(0, ROWS)

    def begin(f):
        def columns(src_e):
            return pl.ds(pl.multiple_of(src_e * COLS + f * HALF, HALF), HALF)

        def pass_on(i, src_e, rows, to):
            part = xb.at[rows, columns(src_e)]
            return far(part, part, ag_s.at[f, i], ag_r.at[f, i], s, to)

        arrive(ob.at[f], rb.at[f], a_r.at[f])
        xb[:, columns(e)] = dot(tight, rb[f].astype(F32).reshape(SLOTS, HALF).astype(BF16)).astype(BF16)
        g = [
            pass_on(0, e, first, ue), pass_on(1, e, second, ue), pass_on(2, e, second, de), pass_on(3, e, first, de),
            pass_on(4, de, first, ue), pass_on(5, ue, second, de),
            pass_on(6, e, every, pe), pass_on(7, de, every, pe), pass_on(8, ue, every, pe), pass_on(9, fe, every, pe),
        ]
        for i in (0, 2, 6, 1, 3):
            g[i].start()
        return g

    def relay_on(g):
        g[0].wait_recv()
        g[4].start()
        g[2].wait_recv()
        g[5].start()

    def share_near(g):
        g[1].wait_recv()
        g[7].start()
        g[3].wait_recv()
        g[8].start()

    def share_far(g):
        g[4].wait_recv()
        g[5].wait_recv()
        g[9].start()

    def absorb(offset, width):
        cols = pl.ds(pl.multiple_of(offset, width), width)
        return dot_nt(xb[:, cols], gu[:, cols])

    gather0 = begin(0)
    ss_p.wait_recv()
    squares = squares + sr[0]
    ss[1] = squares
    ss_z = [far(ss.at[1], sr.at[i], ss_s.at[i], ss_r.at[i], s, to) for i, to in ((1, ue), (2, de), (3, fe))]
    for copy in ss_z:
        copy.start()
    gather1 = begin(1)
    relay_on(gather0)

    for copy in ss_z:
        copy.wait_recv()
    scale_row = lax.rsqrt((squares + sr[1] + sr[2] + sr[3])[0:1, :] / D + EPSILON)
    chosen = jnp.where(iota((NSEQ, TOK), 0).astype(F32) == picked_row, 1.0, 0.0)
    ranked = jnp.where(lane.astype(F32) == rank_col, as_column(scale_row), 0.0)
    osc[...] = exact_dot(chosen, ranked).reshape(NSEQ, 1, TOK)
    scatter(osc, rsc, c_s.at[0], c_r.at[0])

    share_near(gather0)
    for copy in e_loads:
        copy.wait()
    gather0[6].wait_recv()
    gather1[6].wait_recv()
    acc[...] = absorb(zh * 1024, 1024)
    relay_on(gather1)
    share_near(gather1)
    for g in (gather0, gather1):
        g[7].wait_recv()
        g[8].wait_recv()
    acc[...] += absorb((ue // 2) * 1024, 1024)
    share_far(gather0)
    acc[...] += absorb((de // 2) * 1024, 1024)
    gather0[9].wait_recv()
    acc[...] += absorb(fe * COLS, HALF) + absorb(pfe * COLS, HALF)
    share_far(gather1)
    acc[...] += absorb(fe * COLS + HALF, HALF)
    gather1[9].wait_recv()
    acc[...] += absorb(pfe * COLS + HALF, HALF)

    arrive(osc, rsc, c_r.at[0])
    owner = jnp.where(iota((ROWS, NSEQ), 0) // 7 == iota((ROWS, NSEQ), 1), 1.0, 0.0)
    mine = lax.rem(iota((ROWS, TOK), 0), 7) == iota((ROWS, TOK), 1)
    scale = jnp.sum(jnp.where(mine, exact_dot(owner, rsc[...].reshape(NSEQ, TOK)), 0.0), axis=1, keepdims=True)
    gate_sum = acc[:, 0:UNITS] * scale
    up_sum = acc[:, 384:384 + UNITS] * scale
    logit = acc[:, UNITS:UNITS + 1] * scale
    hidden = gate_sum / (1.0 + jnp.exp(-gate_sum)) * up_sum * (1.0 / (1.0 + jnp.exp(-logit)))
    hb[c] = hidden.astype(BF16)
    hid_x = far(hb.at[c], hb.at[c], pair_s.at[1], pair_r.at[1], s, pe)
    hid_x.start()
    for copy in d_loads:
        copy.wait()
    for z in range(4, 8):
        wd[z].wait_recv()
    hid_x.wait_recv()

    def expert_out(z, f):
        cols = slice(f * HALF, (f + 1) * HALF)
        return dot(hb[0], d2[z, 0, :, cols]) + dot(hb[1], d2[z, 1, :, cols])

    def to_tokens(f, left, right):
        yb[f, :, :, :QUART] = dot(loose, left.astype(BF16)).reshape(NSEQ, 8, QUART).astype(BF16)
        yb[f, :, :, QUART:] = dot(loose, right.astype(BF16)).reshape(NSEQ, 8, QUART).astype(BF16)
        scatter(yb.at[f], zb.at[f], b_s.at[f], b_r.at[f])

    r2 = reduced(expert_out, r2s, r2r, r2_s, r2_r, to_tokens)
    for f in range(2):
        cols = slice(f * HALF, (f + 1) * HALF)
        arrive(yb.at[f], zb.at[f], b_r.at[f])
        routed = dot(pick, zb[f].astype(F32).reshape(SLOTS, HALF).astype(BF16))
        out_ref[:, cols] = resid[:, cols] + routed

    for trio in kv:
        for copy in trio:
            copy.wait_send()
    for copy in wd + [att_x, hid_x, *r1, *r2, ss_p, *ss_z, *gather0, *gather1]:
        copy.wait_send()
    for buf, sem in ((ob.at[0], a_s.at[0]), (ob.at[1], a_s.at[1]), (osc, c_s.at[0]), (yb.at[0], b_s.at[0]),
                     (yb.at[1], b_s.at[1])):
        arrive(buf, buf, sem)


def local(
    query_input, key_input, value_input, segment_ids, residual_in, out_weight, norm_gain, router,
    modality, expert_in, gate_weight, up_weight, down_weight,
):
    anywhere = pl.BlockSpec(memory_space=pltpu.HBM)
    vmem = pl.BlockSpec(memory_space=pltpu.VMEM)
    V = pltpu.VMEM
    dma = pltpu.SemaphoreType.DMA
    total = pl.pallas_call(
        kernel,
        out_shape=pltpu.VMEM((TOK, COLS), F32),
        in_specs=[anywhere] * 13,
        out_specs=vmem,
        scratch_shapes=[
            V((TOK, WIDE), BF16),
            V((5, TOK, WIDE), BF16),
            V((5, TOK, WIDE), BF16),
            V((5, 1, TOK), jnp.int32),
            V((1, TOK), jnp.int32),
            V((1, TOK), jnp.int32),
            V((1, COLS), F32),
            V((1, D), BF16),
            V((TOK, COLS), BF16),
            V((4, 2, WIDE, COLS), BF16),
            V((736, D), BF16),
            V((4, 2, UNITS, COLS), BF16),
            V((2, TOK, WIDE), BF16),
            V((2, 6, TOK, QUART), BF16),
            V((2, 6, TOK, QUART), BF16),
            V((2, 8, TOK), F32),
            V((4, 8, TOK), F32),
            V((2, NSEQ, 8, HALF), BF16),
            V((2, NSEQ, 8, HALF), BF16),
            V((NSEQ, 1, TOK), F32),
            V((NSEQ, 1, TOK), F32),
            V((ROWS, D), BF16),
            V((ROWS, 736), F32),
            V((2, ROWS, UNITS), BF16),
            V((2, 6, ROWS, QUART), BF16),
            V((2, 6, ROWS, QUART), BF16),
            V((2, NSEQ, 8, HALF), BF16),
            V((2, NSEQ, 8, HALF), BF16),
            V((TOK, COLS), F32),
            pltpu.SemaphoreType.REGULAR((2,)),
            dma((19,)),
            dma((4, 3)), dma((4, 3)),
            dma((8,)), dma((8,)),
            dma((2,)), dma((2,)),
            dma((2, 6)), dma((2, 6)),
            dma((4,)), dma((4,)),
            dma((2,)), dma((2,)),
            dma((1,)), dma((1,)),
            dma((2, 10)), dma((2, 10)),
            dma((2, 6)), dma((2, 6)),
            dma((2,)), dma((2,)),
        ],
        compiler_params=pltpu.CompilerParams(
            collective_id=0, has_side_effects=True, vmem_limit_bytes=67043328 - 278528),
    )(
        query_input, key_input, value_input, segment_ids.reshape(1, TOK), modality.reshape(1, TOK),
        expert_in.reshape(1, TOK), residual_in, out_weight, norm_gain.reshape(1, COLS),
        router.T, gate_weight[0].T, up_weight[0].T, down_weight[0],
    )
    return total.astype(BF16)


def solution(mesh):
    placed = (
        P("seq", "exp"), P("seq", "exp"), P("seq", "exp"), P("seq"), P("seq", "exp"), P("exp", None), P("exp"),
        P(None, "seq"), P("seq"), P("seq"), P("seq", None, "exp"), P("seq", None, "exp"), P("seq", "exp", None),
    )
    return jax.shard_map(local, mesh=mesh, in_specs=placed, out_specs=P("seq", "exp"), check_vma=False)
```

```python
import jax
import jax.numpy as jnp
from jax import lax
from jax.experimental import pallas as pl
from jax.experimental.pallas import tpu as pltpu
from jax.sharding import PartitionSpec as P

D = 4096
EPSILON = 1e-05
NEGATIVE = -1e30
TOK = 128
HEAD = 128
WIDE = 256
COLS = 512
HALF = 256
QUART = 128
NSEQ = 32
ROWS = 224
SLOTS = 256
UNITS = 352
MESH = pl.DeviceIdType.MESH
F32 = jnp.float32
BF16 = jnp.bfloat16


def dot(a, b):
    return jnp.dot(a, b, preferred_element_type=F32)


def dot_nt(a, b):
    return lax.dot_general(a, b, (((1,), (1,)), ((), ())), preferred_element_type=F32)


def exact_dot(a, b):
    return jnp.dot(a, b, precision=lax.Precision.HIGHEST, preferred_element_type=F32)


def iota(shape, dim):
    return lax.broadcasted_iota(jnp.int32, shape, dim)


def as_column(row):
    return jnp.transpose(jnp.broadcast_to(row, (TOK, TOK)))


def kernel(
    q_hbm, k_hbm, v_hbm, seg_hbm, mod_hbm, pick_hbm, res_hbm, w_hbm, gain_hbm, router_hbm, gate_hbm, up_hbm, down_hbm,
    out_ref,
    qs, kb, vb, sb, mods, picks, gains, rout, res, w2, gu, d2, att, r1s, r1r, ss, sr, ob, rb, osc, rsc, xb, acc, hb,
    r2s, r2r, yb, zb, resid, known, lsem, kv_s, kv_r, wd_s, wd_r, pair_s, pair_r, r1_s, r1_r, ss_s, ss_r, a_s, a_r, c_s, c_r, ag_s, ag_r, r2_s, r2_r, b_s, b_r,
):
    s = lax.axis_index("seq")
    e = lax.axis_index("exp")
    zh = e // 2
    c = e % 2
    other = 1 - c
    pe = zh * 2 + other
    ue = lax.rem(zh + 1, 4) * 2 + c
    de = lax.rem(zh + 3, 4) * 2 + c
    fe = lax.rem(zh + 2, 4) * 2 + c
    pfe = lax.rem(zh + 2, 4) * 2 + other

    def far(src, dst, send, recv, to_s, to_e):
        return pltpu.make_async_remote_copy(
            src_ref=src, dst_ref=dst, send_sem=send, recv_sem=recv,
            device_id={"seq": to_s, "exp": to_e}, device_id_type=MESH,
        )

    def ring(i):
        return lax.rem(s + i + NSEQ, NSEQ)

    def tell(sem, to_s, to_e):
        pl.semaphore_signal(sem, inc=1, device_id={"seq": to_s, "exp": to_e}, device_id_type=MESH)

    barrier = pltpu.get_barrier_semaphore()
    for i in (1, 2, 3, 4, -1, -2, -3, -4):
        tell(barrier, ring(i), e)
    for to in (pe, ue, de):
        tell(barrier, s, to)

    loads = [
        pltpu.make_async_copy(q_hbm, qs, lsem.at[0]),
        pltpu.make_async_copy(k_hbm, kb.at[0], lsem.at[1]),
        pltpu.make_async_copy(v_hbm, vb.at[0], lsem.at[2]),
        pltpu.make_async_copy(seg_hbm, sb.at[0], lsem.at[14]),
    ]
    later = [
        pltpu.make_async_copy(mod_hbm, mods, lsem.at[15]),
        pltpu.make_async_copy(pick_hbm, picks, lsem.at[16]),
        pltpu.make_async_copy(gain_hbm, gains, lsem.at[17]),
        pltpu.make_async_copy(router_hbm, rout, lsem.at[18]),
        pltpu.make_async_copy(res_hbm, res, lsem.at[3]),
    ]
    w_loads = [
        pltpu.make_async_copy(
            w_hbm.at[:, pl.ds(pl.multiple_of(z * 1024 + c * COLS, COLS), COLS)], w2.at[z, c], lsem.at[4 + z])
        for z in range(4)
    ]
    e_loads = [
        pltpu.make_async_copy(gate_hbm, gu.at[pl.ds(0, UNITS)], lsem.at[8]),
        pltpu.make_async_copy(up_hbm, gu.at[pl.ds(384, UNITS)], lsem.at[9]),
    ]
    d_loads = [
        pltpu.make_async_copy(
            down_hbm.at[:, pl.ds(pl.multiple_of(z * 1024 + c * COLS, COLS), COLS)], d2.at[z, c], lsem.at[10 + z])
        for z in range(4)
    ]
    for copy in loads + later + w_loads + e_loads + d_loads:
        copy.start()
    for copy in loads:
        copy.wait()
    pl.semaphore_wait(barrier, 11)

    last = lax.rem(s, 4) == 3

    def trio_of(k, src, to):
        return [
            far(buf.at[src], buf.at[k], kv_s.at[k - 1, j], kv_r.at[k - 1, j], to, e)
            for j, buf in enumerate((sb, kb, vb))
        ]

    kv = [trio_of(k, 0, ring(k)) for k in range(1, 5)]
    relay = trio_of(1, 4, ring(-3))
    for k in (4, 3, 2):
        kv[k - 1][0].start()
    for k in (4, 3, 2):
        kv[k - 1][1].start()
        kv[k - 1][2].start()

    @pl.when(jnp.logical_not(last))
    def _():
        for copy in kv[0]:
            copy.start()

    wd = [
        far(w_hbm.at[:, pl.ds(pl.multiple_of(z * 1024 + other * COLS, COLS), COLS)], w2.at[z, c],
            wd_s.at[z], wd_r.at[z], s, pe)
        for z in range(4)
    ] + [
        far(down_hbm.at[:, pl.ds(pl.multiple_of(z * 1024 + other * COLS, COLS), COLS)], d2.at[z, c],
            wd_s.at[4 + z], wd_r.at[4 + z], s, pe)
        for z in range(4)
    ]
    tell(known.at[0], ring(4), e)
    tell(known.at[0], ring(-4), e)
    for copy in wd:
        copy.start()

    for copy in later:
        copy.wait()
    gu[UNITS:384, :] = jnp.broadcast_to(rout[...].astype(F32), (32, D)).astype(BF16)
    seg_row, picked_row = sb[0].astype(F32), (mods[...] * 16 + picks[...]).astype(F32)
    seg_col = as_column(seg_row)
    picked_col = as_column(picked_row)
    same = picked_col == jnp.broadcast_to(picked_row, (TOK, TOK))
    sub, lane = iota((TOK, TOK), 0), iota((TOK, TOK), 1)
    rank_row = jnp.sum(jnp.where(same & (sub < lane), 1.0, 0.0), axis=0, keepdims=True)
    rank_col = jnp.sum(jnp.where(same & (lane < sub), 1.0, 0.0), axis=1, keepdims=True)
    slot_row = picked_row * 8.0 + rank_row
    slot_col = picked_col[:, 0:1] * 8.0 + rank_col
    spread = jnp.where(iota((SLOTS, TOK), 0).astype(F32) == slot_row, 1.0, 0.0).astype(BF16)
    pick = jnp.where(iota((TOK, SLOTS), 1).astype(F32) == slot_col, 1.0, 0.0).astype(BF16)

    for copy in kv[3]:
        copy.wait_recv()

    @pl.when(last)
    def _():
        for copy in relay:
            copy.start()

    pl.semaphore_wait(known.at[0], 2)
    tell(known.at[1], ring(8), e)
    tell(known.at[1], ring(-8), e)

    scores = [None] * 5
    for k in (0, 4, 3, 2, 1):
        if k == 0:
            allowed = (seg_col == seg_row) & (lane <= sub)
        else:
            if k < 4:
                for copy in kv[k - 1]:
                    copy.wait_recv()
            shift = jnp.where(s >= k, 0.0, 1000.0)
            allowed = seg_col == sb[k].astype(F32) + shift
        both = []
        for h in range(2):
            cols = slice(h * HEAD, (h + 1) * HEAD)
            raw = dot_nt(qs[:, cols], kb[k, :, cols]) * HEAD ** (-0.5)
            both.append(jnp.where(allowed, raw, NEGATIVE))
        scores[k] = both
    for h in range(2):
        cols = slice(h * HEAD, (h + 1) * HEAD)
        top = scores[0][h]
        for k in range(1, 5):
            top = jnp.maximum(top, scores[k][h])
        top = jnp.max(top, axis=1, keepdims=True)
        total = jnp.zeros((TOK, TOK), F32)
        numer = jnp.zeros((TOK, HEAD), F32)
        for k in range(5):
            weight = jnp.exp(scores[k][h] - top)
            total = total + weight
            numer = numer + dot(weight.astype(BF16), vb[k, :, cols])
        denom = jnp.sum(total, axis=1, keepdims=True)
        att[c, :, cols] = (numer / denom).astype(BF16)
    att_x = far(att.at[c], att.at[c], pair_s.at[0], pair_r.at[0], s, pe)
    att_x.start()
    for copy in w_loads:
        copy.wait()
    for z in range(4):
        wd[z].wait_recv()
    att_x.wait_recv()

    def reduced(part, sent, came, sends, recvs, emit):
        copies = []

        def go(f, i, to):
            copy = far(sent.at[f, i], came.at[f, i], sends.at[f, i], recvs.at[f, i], s, to)
            copy.start()
            copies.append(copy)
            return copy

        ahead = []
        for f in range(2):
            value = part(lax.rem(zh + 2, 4), f)
            sent[f, 0] = value[:, :QUART].astype(BF16)
            sent[f, 3] = value[:, QUART:].astype(BF16)
            ahead.append((go(f, 0, ue), go(f, 3, de)))
        waits, owns = [], []
        for f in range(2):
            up_value = part(lax.rem(zh + 1, 4), f)
            sent[f, 1] = up_value[:, QUART:].astype(BF16)
            c1 = go(f, 1, ue)
            down_value = part(lax.rem(zh + 3, 4), f)
            sent[f, 4] = down_value[:, :QUART].astype(BF16)
            c4 = go(f, 4, de)
            owns.append(part(zh, f))
            ahead[f][0].wait_recv()
            sent[f, 2] = (up_value[:, :QUART] + came[f, 0].astype(F32)).astype(BF16)
            c2 = go(f, 2, ue)
            ahead[f][1].wait_recv()
            sent[f, 5] = (down_value[:, QUART:] + came[f, 3].astype(F32)).astype(BF16)
            c5 = go(f, 5, de)
            waits.append((c1, c4, c2, c5))
        for f in range(2):
            for copy in waits[f]:
                copy.wait_recv()
            left = owns[f][:, :QUART] + came[f, 2].astype(F32) + came[f, 4].astype(F32)
            right = owns[f][:, QUART:] + came[f, 1].astype(F32) + came[f, 5].astype(F32)
            emit(f, left, right)
        return copies

    def scatter(outs, ins, send, recv):
        @pl.loop(1, NSEQ)
        def _(i):
            to = lax.rem(s + i, NSEQ)
            far(outs.at[to], ins.at[s], send, recv, to, e).start()

        ins[s] = outs[s]

    def arrive(outs, ins, sem):
        pltpu.make_async_copy(outs.at[pl.ds(0, NSEQ - 1)], ins.at[pl.ds(0, NSEQ - 1)], sem).wait()

    def projected(z, f):
        cols = slice(f * HALF, (f + 1) * HALF)
        return dot(att[0], w2[z, 0, :, cols]) + dot(att[1], w2[z, 1, :, cols])

    partial_squares = []

    def to_experts(f, left, right):
        low, high = slice(f * HALF, f * HALF + QUART), slice(f * HALF + QUART, (f + 1) * HALF)
        left = res[:, low].astype(F32) + left
        right = res[:, high].astype(F32) + right
        resid[:, low] = left
        resid[:, high] = right
        partial_squares.append(left * left + right * right)
        gained = (resid[:, f * HALF:(f + 1) * HALF] * gains[:, f * HALF:(f + 1) * HALF]).astype(BF16)
        ob[f] = dot(spread, gained).reshape(NSEQ, 8, HALF).astype(BF16)
        scatter(ob.at[f], rb.at[f], a_s.at[f], a_r.at[f])

    pl.semaphore_wait(known.at[1], 2)
    r1 = reduced(projected, r1s, r1r, r1_s, r1_r, to_experts)

    squares = jnp.sum(partial_squares[0] + partial_squares[1], axis=1, keepdims=True)
    squares = jnp.transpose(jnp.broadcast_to(squares, (TOK, TOK)))[0:8, :]
    ss[0] = squares
    ss_p = far(ss.at[0], sr.at[0], ss_s.at[0], ss_r.at[0], s, pe)
    ss_p.start()

    row, col = iota((ROWS, SLOTS), 0), iota((ROWS, SLOTS), 1)
    tight = jnp.where((row == (col >> 3) * 7 + (col & 7)) & ((col & 7) < 7), 1.0, 0.0).astype(BF16)
    row, col = iota((SLOTS, ROWS), 0), iota((SLOTS, ROWS), 1)
    loose = jnp.where((col == (row >> 3) * 7 + (row & 7)) & ((row & 7) < 7), 1.0, 0.0).astype(BF16)

    first, second = pl.ds(0, ROWS // 2), pl.ds(ROWS // 2, ROWS // 2)
    every = pl.ds(0, ROWS)

    def begin(f):
        def columns(src_e):
            return pl.ds(pl.multiple_of(src_e * COLS + f * HALF, HALF), HALF)

        def pass_on(i, src_e, rows, to):
            part = xb.at[rows, columns(src_e)]
            return far(part, part, ag_s.at[f, i], ag_r.at[f, i], s, to)

        arrive(ob.at[f], rb.at[f], a_r.at[f])
        xb[:, columns(e)] = dot(tight, rb[f].astype(F32).reshape(SLOTS, HALF).astype(BF16)).astype(BF16)
        g = [
            pass_on(0, e, first, ue), pass_on(1, e, second, ue), pass_on(2, e, second, de), pass_on(3, e, first, de),
            pass_on(4, de, first, ue), pass_on(5, ue, second, de),
            pass_on(6, e, every, pe), pass_on(7, de, every, pe), pass_on(8, ue, every, pe), pass_on(9, fe, every, pe),
        ]
        for i in (0, 2, 6, 1, 3):
            g[i].start()
        return g

    def relay_on(g):
        g[0].wait_recv()
        g[4].start()
        g[2].wait_recv()
        g[5].start()

    def share_near(g):
        g[1].wait_recv()
        g[7].start()
        g[3].wait_recv()
        g[8].start()

    def share_far(g):
        g[4].wait_recv()
        g[5].wait_recv()
        g[9].start()

    def absorb(offset, width):
        cols = pl.ds(pl.multiple_of(offset, width), width)
        return dot_nt(xb[:, cols], gu[:, cols])

    ss_p.wait_recv()
    squares = squares + sr[0]
    ss[1] = squares
    ss_z = [far(ss.at[1], sr.at[i], ss_s.at[i], ss_r.at[i], s, to) for i, to in ((3, fe), (1, ue), (2, de))]
    for copy in ss_z:
        copy.start()
    gather0 = begin(0)

    for copy in ss_z:
        copy.wait_recv()
    scale_row = lax.rsqrt((squares + sr[1] + sr[2] + sr[3])[0:1, :] / D + EPSILON)
    chosen = jnp.where(iota((NSEQ, TOK), 0).astype(F32) == picked_row, 1.0, 0.0)
    ranked = jnp.where(lane.astype(F32) == rank_col, as_column(scale_row), 0.0)
    osc[...] = exact_dot(chosen, ranked).reshape(NSEQ, 1, TOK)
    scatter(osc, rsc, c_s.at[0], c_r.at[0])

    gather1 = begin(1)
    relay_on(gather0)
    share_near(gather0)
    for copy in e_loads:
        copy.wait()
    gather0[6].wait_recv()
    gather1[6].wait_recv()
    acc[...] = absorb(zh * 1024, 1024)
    relay_on(gather1)
    share_near(gather1)
    for g in (gather0, gather1):
        g[7].wait_recv()
        g[8].wait_recv()
    acc[...] += absorb((ue // 2) * 1024, 1024)
    share_far(gather0)
    acc[...] += absorb((de // 2) * 1024, 1024)
    gather0[9].wait_recv()
    acc[...] += absorb(fe * COLS, HALF) + absorb(pfe * COLS, HALF)
    share_far(gather1)
    acc[...] += absorb(fe * COLS + HALF, HALF)
    gather1[9].wait_recv()
    acc[...] += absorb(pfe * COLS + HALF, HALF)

    arrive(osc, rsc, c_r.at[0])
    owner = jnp.where(iota((ROWS, NSEQ), 0) // 7 == iota((ROWS, NSEQ), 1), 1.0, 0.0)
    mine = lax.rem(iota((ROWS, TOK), 0), 7) == iota((ROWS, TOK), 1)
    scale = jnp.sum(jnp.where(mine, exact_dot(owner, rsc[...].reshape(NSEQ, TOK)), 0.0), axis=1, keepdims=True)
    gate_sum = acc[:, 0:UNITS] * scale
    up_sum = acc[:, 384:384 + UNITS] * scale
    logit = acc[:, UNITS:UNITS + 1] * scale
    hidden = gate_sum / (1.0 + jnp.exp(-gate_sum)) * up_sum * (1.0 / (1.0 + jnp.exp(-logit)))
    hb[c] = hidden.astype(BF16)
    hid_x = far(hb.at[c], hb.at[c], pair_s.at[1], pair_r.at[1], s, pe)
    hid_x.start()
    for copy in d_loads:
        copy.wait()
    for z in range(4, 8):
        wd[z].wait_recv()
    hid_x.wait_recv()

    def expert_out(z, f):
        cols = slice(f * HALF, (f + 1) * HALF)
        return dot(hb[0], d2[z, 0, :, cols]) + dot(hb[1], d2[z, 1, :, cols])

    def to_tokens(f, left, right):
        yb[f, :, :, :QUART] = dot(loose, left.astype(BF16)).reshape(NSEQ, 8, QUART).astype(BF16)
        yb[f, :, :, QUART:] = dot(loose, right.astype(BF16)).reshape(NSEQ, 8, QUART).astype(BF16)
        scatter(yb.at[f], zb.at[f], b_s.at[f], b_r.at[f])

    r2 = reduced(expert_out, r2s, r2r, r2_s, r2_r, to_tokens)
    for f in range(2):
        cols = slice(f * HALF, (f + 1) * HALF)
        arrive(yb.at[f], zb.at[f], b_r.at[f])
        routed = dot(pick, zb[f].astype(F32).reshape(SLOTS, HALF).astype(BF16))
        out_ref[:, cols] = resid[:, cols] + routed

    for trio in kv:
        for copy in trio:
            copy.wait_send()
    for copy in wd + [att_x, hid_x, *r1, *r2, ss_p, *ss_z, *gather0, *gather1]:
        copy.wait_send()
    for buf, sem in ((ob.at[0], a_s.at[0]), (ob.at[1], a_s.at[1]), (osc, c_s.at[0]), (yb.at[0], b_s.at[0]),
                     (yb.at[1], b_s.at[1])):
        arrive(buf, buf, sem)


def local(
    query_input, key_input, value_input, segment_ids, residual_in, out_weight, norm_gain, router,
    modality, expert_in, gate_weight, up_weight, down_weight,
):
    anywhere = pl.BlockSpec(memory_space=pltpu.HBM)
    vmem = pl.BlockSpec(memory_space=pltpu.VMEM)
    V = pltpu.VMEM
    dma = pltpu.SemaphoreType.DMA
    total = pl.pallas_call(
        kernel,
        out_shape=pltpu.VMEM((TOK, COLS), F32),
        in_specs=[anywhere] * 13,
        out_specs=vmem,
        scratch_shapes=[
            V((TOK, WIDE), BF16),
            V((5, TOK, WIDE), BF16),
            V((5, TOK, WIDE), BF16),
            V((5, 1, TOK), jnp.int32),
            V((1, TOK), jnp.int32),
            V((1, TOK), jnp.int32),
            V((1, COLS), F32),
            V((1, D), BF16),
            V((TOK, COLS), BF16),
            V((4, 2, WIDE, COLS), BF16),
            V((736, D), BF16),
            V((4, 2, UNITS, COLS), BF16),
            V((2, TOK, WIDE), BF16),
            V((2, 6, TOK, QUART), BF16),
            V((2, 6, TOK, QUART), BF16),
            V((2, 8, TOK), F32),
            V((4, 8, TOK), F32),
            V((2, NSEQ, 8, HALF), BF16),
            V((2, NSEQ, 8, HALF), BF16),
            V((NSEQ, 1, TOK), F32),
            V((NSEQ, 1, TOK), F32),
            V((ROWS, D), BF16),
            V((ROWS, 736), F32),
            V((2, ROWS, UNITS), BF16),
            V((2, 6, ROWS, QUART), BF16),
            V((2, 6, ROWS, QUART), BF16),
            V((2, NSEQ, 8, HALF), BF16),
            V((2, NSEQ, 8, HALF), BF16),
            V((TOK, COLS), F32),
            pltpu.SemaphoreType.REGULAR((2,)),
            dma((19,)),
            dma((4, 3)), dma((4, 3)),
            dma((8,)), dma((8,)),
            dma((2,)), dma((2,)),
            dma((2, 6)), dma((2, 6)),
            dma((4,)), dma((4,)),
            dma((2,)), dma((2,)),
            dma((1,)), dma((1,)),
            dma((2, 10)), dma((2, 10)),
            dma((2, 6)), dma((2, 6)),
            dma((2,)), dma((2,)),
        ],
        compiler_params=pltpu.CompilerParams(
            collective_id=0, has_side_effects=True, vmem_limit_bytes=67043328 - 278528),
    )(
        query_input, key_input, value_input, segment_ids.reshape(1, TOK), modality.reshape(1, TOK),
        expert_in.reshape(1, TOK), residual_in, out_weight, norm_gain.reshape(1, COLS),
        router.T, gate_weight[0].T, up_weight[0].T, down_weight[0],
    )
    return total.astype(BF16)


def solution(mesh):
    placed = (
        P("seq", "exp"), P("seq", "exp"), P("seq", "exp"), P("seq"), P("seq", "exp"), P("exp", None), P("exp"),
        P(None, "seq"), P("seq"), P("seq"), P("seq", None, "exp"), P("seq", None, "exp"), P("seq", "exp", None),
    )
    return jax.shard_map(local, mesh=mesh, in_specs=placed, out_specs=P("seq", "exp"), check_vma=False)
```

```python
import jax
import jax.numpy as jnp
from jax import lax
from jax.experimental import pallas as pl
from jax.experimental.pallas import tpu as pltpu
from jax.sharding import PartitionSpec as P

D = 4096
EPSILON = 1e-05
NEGATIVE = -1e30
TOK = 128
HEAD = 128
WIDE = 256
COLS = 512
HALF = 256
QUART = 128
NSEQ = 32
ROWS = 224
SLOTS = 256
UNITS = 352
MESH = pl.DeviceIdType.MESH
F32 = jnp.float32
BF16 = jnp.bfloat16


def dot(a, b):
    return jnp.dot(a, b, preferred_element_type=F32)


def dot_nt(a, b):
    return lax.dot_general(a, b, (((1,), (1,)), ((), ())), preferred_element_type=F32)


def exact_dot(a, b):
    return jnp.dot(a, b, precision=lax.Precision.HIGHEST, preferred_element_type=F32)


def iota(shape, dim):
    return lax.broadcasted_iota(jnp.int32, shape, dim)


def as_column(row):
    return jnp.transpose(jnp.broadcast_to(row, (TOK, TOK)))


def kernel(
    q_hbm, k_hbm, v_hbm, seg_hbm, mod_hbm, pick_hbm, res_hbm, w_hbm, gain_hbm, router_hbm, gate_hbm, up_hbm, down_hbm,
    out_ref,
    qs, kb, vb, sb, mods, picks, gains, rout, res, w2, gu, d2, att, r1s, r1r, ss, sr, ob, rb, osc, rsc, xb, acc, hb,
    r2s, r2r, yb, zb, resid, known, lsem, kv_s, kv_r, wd_s, wd_r, pair_s, pair_r, r1_s, r1_r, ss_s, ss_r, a_s, a_r, c_s, c_r, ag_s, ag_r, r2_s, r2_r, b_s, b_r,
):
    s = lax.axis_index("seq")
    e = lax.axis_index("exp")
    zh = e // 2
    c = e % 2
    other = 1 - c
    pe = zh * 2 + other
    ue = lax.rem(zh + 1, 4) * 2 + c
    de = lax.rem(zh + 3, 4) * 2 + c
    fe = lax.rem(zh + 2, 4) * 2 + c
    pfe = lax.rem(zh + 2, 4) * 2 + other

    def far(src, dst, send, recv, to_s, to_e):
        return pltpu.make_async_remote_copy(
            src_ref=src, dst_ref=dst, send_sem=send, recv_sem=recv,
            device_id={"seq": to_s, "exp": to_e}, device_id_type=MESH,
        )

    def ring(i):
        return lax.rem(s + i + NSEQ, NSEQ)

    def tell(sem, to_s, to_e):
        pl.semaphore_signal(sem, inc=1, device_id={"seq": to_s, "exp": to_e}, device_id_type=MESH)

    barrier = pltpu.get_barrier_semaphore()
    for i in (1, 2, 3, 4, -1, -2, -3, -4):
        tell(barrier, ring(i), e)
    for to in (pe, ue, de):
        tell(barrier, s, to)

    loads = [
        pltpu.make_async_copy(q_hbm, qs, lsem.at[0]),
        pltpu.make_async_copy(k_hbm, kb.at[0], lsem.at[1]),
        pltpu.make_async_copy(v_hbm, vb.at[0], lsem.at[2]),
        pltpu.make_async_copy(seg_hbm, sb.at[0], lsem.at[14]),
    ]
    later = [
        pltpu.make_async_copy(mod_hbm, mods, lsem.at[15]),
        pltpu.make_async_copy(pick_hbm, picks, lsem.at[16]),
        pltpu.make_async_copy(gain_hbm, gains, lsem.at[17]),
        pltpu.make_async_copy(router_hbm, rout, lsem.at[18]),
        pltpu.make_async_copy(res_hbm, res, lsem.at[3]),
    ]
    w_loads = [
        pltpu.make_async_copy(
            w_hbm.at[:, pl.ds(pl.multiple_of(z * 1024 + c * COLS, COLS), COLS)], w2.at[z, c], lsem.at[4 + z])
        for z in range(4)
    ]
    e_loads = [
        pltpu.make_async_copy(gate_hbm, gu.at[pl.ds(0, UNITS)], lsem.at[8]),
        pltpu.make_async_copy(up_hbm, gu.at[pl.ds(384, UNITS)], lsem.at[9]),
    ]
    d_loads = [
        pltpu.make_async_copy(
            down_hbm.at[:, pl.ds(pl.multiple_of(z * 1024 + c * COLS, COLS), COLS)], d2.at[z, c], lsem.at[10 + z])
        for z in range(4)
    ]
    for copy in loads + later + w_loads + e_loads + d_loads:
        copy.start()
    for copy in loads:
        copy.wait()
    pl.semaphore_wait(barrier, 11)

    last = lax.rem(s, 4) == 3

    def trio_of(k, src, to):
        return [
            far(buf.at[src], buf.at[k], kv_s.at[k - 1, j], kv_r.at[k - 1, j], to, e)
            for j, buf in enumerate((sb, kb, vb))
        ]

    kv = [trio_of(k, 0, ring(k)) for k in range(1, 5)]
    relay = trio_of(1, 4, ring(-3))
    for k in (4, 3, 2):
        kv[k - 1][0].start()
    for k in (4, 3, 2):
        kv[k - 1][1].start()
        kv[k - 1][2].start()

    @pl.when(jnp.logical_not(last))
    def _():
        for copy in kv[0]:
            copy.start()

    wd = [
        far(w_hbm.at[:, pl.ds(pl.multiple_of(z * 1024 + other * COLS, COLS), COLS)], w2.at[z, c],
            wd_s.at[z], wd_r.at[z], s, pe)
        for z in range(4)
    ] + [
        far(down_hbm.at[:, pl.ds(pl.multiple_of(z * 1024 + other * COLS, COLS), COLS)], d2.at[z, c],
            wd_s.at[4 + z], wd_r.at[4 + z], s, pe)
        for z in range(4)
    ]
    tell(known.at[0], ring(4), e)
    tell(known.at[0], ring(-4), e)
    for copy in wd:
        copy.start()

    for copy in later:
        copy.wait()
    gu[UNITS:384, :] = jnp.broadcast_to(rout[...].astype(F32), (32, D)).astype(BF16)
    seg_row, picked_row = sb[0].astype(F32), (mods[...] * 16 + picks[...]).astype(F32)
    seg_col = as_column(seg_row)
    picked_col = as_column(picked_row)
    same = picked_col == jnp.broadcast_to(picked_row, (TOK, TOK))
    sub, lane = iota((TOK, TOK), 0), iota((TOK, TOK), 1)
    rank_row = jnp.sum(jnp.where(same & (sub < lane), 1.0, 0.0), axis=0, keepdims=True)
    rank_col = jnp.sum(jnp.where(same & (lane < sub), 1.0, 0.0), axis=1, keepdims=True)
    slot_row = picked_row * 8.0 + rank_row
    slot_col = picked_col[:, 0:1] * 8.0 + rank_col
    spread = jnp.where(iota((SLOTS, TOK), 0).astype(F32) == slot_row, 1.0, 0.0).astype(BF16)
    pick = jnp.where(iota((TOK, SLOTS), 1).astype(F32) == slot_col, 1.0, 0.0).astype(BF16)

    for copy in kv[3]:
        copy.wait_recv()

    @pl.when(last)
    def _():
        for copy in relay:
            copy.start()

    pl.semaphore_wait(known.at[0], 2)
    tell(known.at[1], ring(8), e)
    tell(known.at[1], ring(-8), e)

    scores = [None] * 5
    for k in (0, 4, 3, 2, 1):
        if k == 0:
            allowed = (seg_col == seg_row) & (lane <= sub)
        else:
            if k < 4:
                for copy in kv[k - 1]:
                    copy.wait_recv()
            shift = jnp.where(s >= k, 0.0, 1000.0)
            allowed = seg_col == sb[k].astype(F32) + shift
        both = []
        for h in range(2):
            cols = slice(h * HEAD, (h + 1) * HEAD)
            raw = dot_nt(qs[:, cols], kb[k, :, cols]) * HEAD ** (-0.5)
            both.append(jnp.where(allowed, raw, NEGATIVE))
        scores[k] = both
    for h in range(2):
        cols = slice(h * HEAD, (h + 1) * HEAD)
        top = scores[0][h]
        for k in range(1, 5):
            top = jnp.maximum(top, scores[k][h])
        top = jnp.max(top, axis=1, keepdims=True)
        total = jnp.zeros((TOK, TOK), F32)
        numer = jnp.zeros((TOK, HEAD), F32)
        for k in range(5):
            weight = jnp.exp(scores[k][h] - top)
            total = total + weight
            numer = numer + dot(weight.astype(BF16), vb[k, :, cols])
        denom = jnp.sum(total, axis=1, keepdims=True)
        att[c, :, cols] = (numer / denom).astype(BF16)
    att_x = far(att.at[c], att.at[c], pair_s.at[0], pair_r.at[0], s, pe)
    att_x.start()
    for copy in w_loads:
        copy.wait()
    for z in range(4):
        wd[z].wait_recv()
    att_x.wait_recv()

    def reduced(part, sent, came, sends, recvs, emit):
        copies = []

        def go(f, i, to):
            copy = far(sent.at[f, i], came.at[f, i], sends.at[f, i], recvs.at[f, i], s, to)
            copy.start()
            copies.append(copy)
            return copy

        ahead = []
        for f in range(2):
            value = part(lax.rem(zh + 2, 4), f)
            sent[f, 0] = value[:, :QUART].astype(BF16)
            sent[f, 3] = value[:, QUART:].astype(BF16)
            ahead.append((go(f, 0, ue), go(f, 3, de)))
        waits, owns = [], []
        for f in range(2):
            up_value = part(lax.rem(zh + 1, 4), f)
            sent[f, 1] = up_value[:, QUART:].astype(BF16)
            c1 = go(f, 1, ue)
            down_value = part(lax.rem(zh + 3, 4), f)
            sent[f, 4] = down_value[:, :QUART].astype(BF16)
            c4 = go(f, 4, de)
            owns.append(part(zh, f))
            ahead[f][0].wait_recv()
            sent[f, 2] = (up_value[:, :QUART] + came[f, 0].astype(F32)).astype(BF16)
            c2 = go(f, 2, ue)
            ahead[f][1].wait_recv()
            sent[f, 5] = (down_value[:, QUART:] + came[f, 3].astype(F32)).astype(BF16)
            c5 = go(f, 5, de)
            waits.append((c1, c4, c2, c5))
        for f in range(2):
            for copy in waits[f]:
                copy.wait_recv()
            left = owns[f][:, :QUART] + came[f, 2].astype(F32) + came[f, 4].astype(F32)
            right = owns[f][:, QUART:] + came[f, 1].astype(F32) + came[f, 5].astype(F32)
            emit(f, left, right)
        return copies

    def scatter(outs, ins, send, recv):
        @pl.loop(1, NSEQ)
        def _(i):
            to = lax.rem(s + lax.rem(i + 11, NSEQ - 1) + 1, NSEQ)
            far(outs.at[to], ins.at[s], send, recv, to, e).start()

        ins[s] = outs[s]

    def arrive(outs, ins, sem):
        pltpu.make_async_copy(outs.at[pl.ds(0, NSEQ - 1)], ins.at[pl.ds(0, NSEQ - 1)], sem).wait()

    def projected(z, f):
        cols = slice(f * HALF, (f + 1) * HALF)
        return dot(att[0], w2[z, 0, :, cols]) + dot(att[1], w2[z, 1, :, cols])

    partial_squares = []

    def to_experts(f, left, right):
        low, high = slice(f * HALF, f * HALF + QUART), slice(f * HALF + QUART, (f + 1) * HALF)
        left = res[:, low].astype(F32) + left
        right = res[:, high].astype(F32) + right
        resid[:, low] = left
        resid[:, high] = right
        partial_squares.append(left * left + right * right)
        gained = (resid[:, f * HALF:(f + 1) * HALF] * gains[:, f * HALF:(f + 1) * HALF]).astype(BF16)
        ob[f] = dot(spread, gained).reshape(NSEQ, 8, HALF).astype(BF16)
        scatter(ob.at[f], rb.at[f], a_s.at[f], a_r.at[f])

    pl.semaphore_wait(known.at[1], 2)
    r1 = reduced(projected, r1s, r1r, r1_s, r1_r, to_experts)

    squares = jnp.sum(partial_squares[0] + partial_squares[1], axis=1, keepdims=True)
    squares = jnp.transpose(jnp.broadcast_to(squares, (TOK, TOK)))[0:8, :]
    ss[0] = squares
    ss_p = far(ss.at[0], sr.at[0], ss_s.at[0], ss_r.at[0], s, pe)
    ss_p.start()

    row, col = iota((ROWS, SLOTS), 0), iota((ROWS, SLOTS), 1)
    tight = jnp.where((row == (col >> 3) * 7 + (col & 7)) & ((col & 7) < 7), 1.0, 0.0).astype(BF16)
    row, col = iota((SLOTS, ROWS), 0), iota((SLOTS, ROWS), 1)
    loose = jnp.where((col == (row >> 3) * 7 + (row & 7)) & ((row & 7) < 7), 1.0, 0.0).astype(BF16)

    first, second = pl.ds(0, ROWS // 2), pl.ds(ROWS // 2, ROWS // 2)
    every = pl.ds(0, ROWS)

    def begin(f):
        def columns(src_e):
            return pl.ds(pl.multiple_of(src_e * COLS + f * HALF, HALF), HALF)

        def pass_on(i, src_e, rows, to):
            part = xb.at[rows, columns(src_e)]
            return far(part, part, ag_s.at[f, i], ag_r.at[f, i], s, to)

        arrive(ob.at[f], rb.at[f], a_r.at[f])
        xb[:, columns(e)] = dot(tight, rb[f].astype(F32).reshape(SLOTS, HALF).astype(BF16)).astype(BF16)
        g = [
            pass_on(0, e, first, ue), pass_on(1, e, second, ue), pass_on(2, e, second, de), pass_on(3, e, first, de),
            pass_on(4, de, first, ue), pass_on(5, ue, second, de),
            pass_on(6, e, every, pe), pass_on(7, de, every, pe), pass_on(8, ue, every, pe), pass_on(9, fe, every, pe),
        ]
        for i in (0, 2, 6, 1, 3):
            g[i].start()
        return g

    def relay_on(g):
        g[0].wait_recv()
        g[4].start()
        g[2].wait_recv()
        g[5].start()

    def share_near(g):
        g[1].wait_recv()
        g[7].start()
        g[3].wait_recv()
        g[8].start()

    def share_far(g):
        g[4].wait_recv()
        g[5].wait_recv()
        g[9].start()

    def absorb(offset, width):
        cols = pl.ds(pl.multiple_of(offset, width), width)
        return dot_nt(xb[:, cols], gu[:, cols])

    ss_p.wait_recv()
    squares = squares + sr[0]
    ss[1] = squares
    ss_z = [far(ss.at[1], sr.at[i], ss_s.at[i], ss_r.at[i], s, to) for i, to in ((3, fe), (1, ue), (2, de))]
    for copy in ss_z:
        copy.start()
    gather0 = begin(0)

    for copy in ss_z:
        copy.wait_recv()
    scale_row = lax.rsqrt((squares + sr[1] + sr[2] + sr[3])[0:1, :] / D + EPSILON)
    chosen = jnp.where(iota((NSEQ, TOK), 0).astype(F32) == picked_row, 1.0, 0.0)
    ranked = jnp.where(lane.astype(F32) == rank_col, as_column(scale_row), 0.0)
    osc[...] = exact_dot(chosen, ranked).reshape(NSEQ, 1, TOK)
    scatter(osc, rsc, c_s.at[0], c_r.at[0])

    gather1 = begin(1)
    relay_on(gather0)
    share_near(gather0)
    for copy in e_loads:
        copy.wait()
    gather0[6].wait_recv()
    gather1[6].wait_recv()
    acc[...] = absorb(zh * 1024, 1024)
    relay_on(gather1)
    share_near(gather1)
    for g in (gather0, gather1):
        g[7].wait_recv()
        g[8].wait_recv()
    acc[...] += absorb((ue // 2) * 1024, 1024)
    share_far(gather0)
    acc[...] += absorb((de // 2) * 1024, 1024)
    gather0[9].wait_recv()
    acc[...] += absorb(fe * COLS, HALF) + absorb(pfe * COLS, HALF)
    share_far(gather1)
    acc[...] += absorb(fe * COLS + HALF, HALF)
    gather1[9].wait_recv()
    acc[...] += absorb(pfe * COLS + HALF, HALF)

    arrive(osc, rsc, c_r.at[0])
    owner = jnp.where(iota((ROWS, NSEQ), 0) // 7 == iota((ROWS, NSEQ), 1), 1.0, 0.0)
    mine = lax.rem(iota((ROWS, TOK), 0), 7) == iota((ROWS, TOK), 1)
    scale = jnp.sum(jnp.where(mine, exact_dot(owner, rsc[...].reshape(NSEQ, TOK)), 0.0), axis=1, keepdims=True)
    gate_sum = acc[:, 0:UNITS] * scale
    up_sum = acc[:, 384:384 + UNITS] * scale
    logit = acc[:, UNITS:UNITS + 1] * scale
    hidden = gate_sum / (1.0 + jnp.exp(-gate_sum)) * up_sum * (1.0 / (1.0 + jnp.exp(-logit)))
    hb[c] = hidden.astype(BF16)
    hid_x = far(hb.at[c], hb.at[c], pair_s.at[1], pair_r.at[1], s, pe)
    hid_x.start()
    for copy in d_loads:
        copy.wait()
    for z in range(4, 8):
        wd[z].wait_recv()
    hid_x.wait_recv()

    def expert_out(z, f):
        cols = slice(f * HALF, (f + 1) * HALF)
        return dot(hb[0], d2[z, 0, :, cols]) + dot(hb[1], d2[z, 1, :, cols])

    def to_tokens(f, left, right):
        yb[f, :, :, :QUART] = dot(loose, left.astype(BF16)).reshape(NSEQ, 8, QUART).astype(BF16)
        yb[f, :, :, QUART:] = dot(loose, right.astype(BF16)).reshape(NSEQ, 8, QUART).astype(BF16)
        scatter(yb.at[f], zb.at[f], b_s.at[f], b_r.at[f])

    r2 = reduced(expert_out, r2s, r2r, r2_s, r2_r, to_tokens)
    for f in range(2):
        cols = slice(f * HALF, (f + 1) * HALF)
        arrive(yb.at[f], zb.at[f], b_r.at[f])
        routed = dot(pick, zb[f].astype(F32).reshape(SLOTS, HALF).astype(BF16))
        out_ref[:, cols] = resid[:, cols] + routed

    for trio in kv:
        for copy in trio:
            copy.wait_send()
    for copy in wd + [att_x, hid_x, *r1, *r2, ss_p, *ss_z, *gather0, *gather1]:
        copy.wait_send()
    for buf, sem in ((ob.at[0], a_s.at[0]), (ob.at[1], a_s.at[1]), (osc, c_s.at[0]), (yb.at[0], b_s.at[0]),
                     (yb.at[1], b_s.at[1])):
        arrive(buf, buf, sem)


def local(
    query_input, key_input, value_input, segment_ids, residual_in, out_weight, norm_gain, router,
    modality, expert_in, gate_weight, up_weight, down_weight,
):
    anywhere = pl.BlockSpec(memory_space=pltpu.HBM)
    vmem = pl.BlockSpec(memory_space=pltpu.VMEM)
    V = pltpu.VMEM
    dma = pltpu.SemaphoreType.DMA
    total = pl.pallas_call(
        kernel,
        out_shape=pltpu.VMEM((TOK, COLS), F32),
        in_specs=[anywhere] * 13,
        out_specs=vmem,
        scratch_shapes=[
            V((TOK, WIDE), BF16),
            V((5, TOK, WIDE), BF16),
            V((5, TOK, WIDE), BF16),
            V((5, 1, TOK), jnp.int32),
            V((1, TOK), jnp.int32),
            V((1, TOK), jnp.int32),
            V((1, COLS), F32),
            V((1, D), BF16),
            V((TOK, COLS), BF16),
            V((4, 2, WIDE, COLS), BF16),
            V((736, D), BF16),
            V((4, 2, UNITS, COLS), BF16),
            V((2, TOK, WIDE), BF16),
            V((2, 6, TOK, QUART), BF16),
            V((2, 6, TOK, QUART), BF16),
            V((2, 8, TOK), F32),
            V((4, 8, TOK), F32),
            V((2, NSEQ, 8, HALF), BF16),
            V((2, NSEQ, 8, HALF), BF16),
            V((NSEQ, 1, TOK), F32),
            V((NSEQ, 1, TOK), F32),
            V((ROWS, D), BF16),
            V((ROWS, 736), F32),
            V((2, ROWS, UNITS), BF16),
            V((2, 6, ROWS, QUART), BF16),
            V((2, 6, ROWS, QUART), BF16),
            V((2, NSEQ, 8, HALF), BF16),
            V((2, NSEQ, 8, HALF), BF16),
            V((TOK, COLS), F32),
            pltpu.SemaphoreType.REGULAR((2,)),
            dma((19,)),
            dma((4, 3)), dma((4, 3)),
            dma((8,)), dma((8,)),
            dma((2,)), dma((2,)),
            dma((2, 6)), dma((2, 6)),
            dma((4,)), dma((4,)),
            dma((2,)), dma((2,)),
            dma((1,)), dma((1,)),
            dma((2, 10)), dma((2, 10)),
            dma((2, 6)), dma((2, 6)),
            dma((2,)), dma((2,)),
        ],
        compiler_params=pltpu.CompilerParams(
            collective_id=0, has_side_effects=True, vmem_limit_bytes=67043328 - 278528),
    )(
        query_input, key_input, value_input, segment_ids.reshape(1, TOK), modality.reshape(1, TOK),
        expert_in.reshape(1, TOK), residual_in, out_weight, norm_gain.reshape(1, COLS),
        router.T, gate_weight[0].T, up_weight[0].T, down_weight[0],
    )
    return total.astype(BF16)


def solution(mesh):
    placed = (
        P("seq", "exp"), P("seq", "exp"), P("seq", "exp"), P("seq"), P("seq", "exp"), P("exp", None), P("exp"),
        P(None, "seq"), P("seq"), P("seq"), P("seq", None, "exp"), P("seq", None, "exp"), P("seq", "exp", None),
    )
    return jax.shard_map(local, mesh=mesh, in_specs=placed, out_specs=P("seq", "exp"), check_vma=False)
```
